32 devices in a mesh: img: 2 (over x), rows: 16 (over z, y, core).
Axes of the slice: x: 2, y: 2, z: 4, core: 2. Of those that a mesh axis runs over, the one named last changes fastest.
Arguments:
- hidden_states: bfloat16 [3, 4096, 1024], P(None, ('img', 'rows')), parts along dimension 1, may hold values from -6 to 6
- cell_of: int32 [2048], replicated, may hold values from 0 to 2047, as said below
- proj_four_weight: bfloat16 [1024, 256], replicated, may hold values from -0.1875 to 0.1875
- proj_four_bias: float32 [256], replicated, may hold values from -3 to 3
- proj_two_weight: bfloat16 [1024, 512], replicated, may hold values from -0.1875 to 0.1875
- proj_two_bias: float32 [512], replicated, may hold values from -3 to 3
- proj_same_weight: bfloat16 [1024, 1024], replicated, may hold values from -0.1875 to 0.1875
- proj_same_bias: float32 [1024], replicated, may hold values from -3 to 3
- up4_weight: bfloat16 [256, 4096], replicated, may hold values from -0.375 to 0.375
- up4_bias: float32 [256], replicated, may hold values from -3 to 3
- up2_weight: bfloat16 [512, 2048], replicated, may hold values from -0.25 to 0.25
- up2_bias: float32 [512], replicated, may hold values from -3 to 3
- join_weight: bfloat16 [3, 3, 256, 256], replicated, may hold values from -0.125 to 0.125
Outputs:
- joined_four: bfloat16 [256, 256, 256], P(('img', 'rows')), parts along dimension 0
- upsampled_two: bfloat16 [128, 128, 512], P(('img', 'rows')), parts along dimension 0
- same_scale: bfloat16 [64, 64, 1024], P(('img', 'rows')), parts along dimension 0
The draws below stay inside these ranges and needn't reach their ends.
There are 2 independent parts, one for each index of `img`. The reference program is written for one: setup_inputs(seed, part) draws one part's arguments, and reference() takes and returns one part's arrays. A program takes and returns all parts, laid end to end along the dimension named above; an argument that names none is the same for every part. Nothing has to cross between parts.
Inputs may be any that keep to these rules, and one draw needn't show every extreme that they name: `cell_of`: a permutation of the cells 0 to 2047; the sequence positions k * 128 to (k + 1) * 128 - 1 hold exactly 8 cells of every block of 128 consecutive cells.
All inputs are finite; a program needn't handle non-finite values.
Results may differ from the reference program's by a relative error of at most 0.0057.
Values may be sent and summed in bfloat16 or wider, within the bound.
A program may use at most 64 MiB of HBM per device.

```python
import jax
import jax.numpy as jnp

HOOKS = 3
HID = 1024
C_FOUR = 256
C_TWO = 512
C_SAME = 1024
FEAT = 256
GRID_W = 64
TOK_DEV = 128
GRID_H = 32
TOKENS = 2048


def draw_cell_of(key, part):
    tile_count = TOKENS // TOK_DEV
    per_tile = TOK_DEV // tile_count
    first_key, second_key = jax.random.split(jax.random.fold_in(key, 11))
    base_cells = jnp.arange(TOKENS, dtype=jnp.int32).reshape(tile_count, TOK_DEV)
    shuffled = jax.random.permutation(first_key, base_cells, axis=1, independent=True)
    dealt = shuffled.reshape(tile_count, tile_count, per_tile).transpose(1, 0, 2).reshape(tile_count, TOK_DEV)
    return jax.random.permutation(second_key, dealt, axis=1, independent=True).reshape(TOKENS)


def levels(own_key, dims, cuts, smallest, largest):
    def one(position, blocks):
        steps = jax.random.uniform(jax.random.fold_in(jax.random.fold_in(own_key, 6), position), (blocks,), jnp.float32, smallest / len(cuts), largest / len(cuts))
        return jnp.repeat(jnp.exp(steps), dims[position] // blocks).reshape((-1,) + (1,) * (len(dims) - position - 1))

    loudness = one(*cuts[0])
    for cut in cuts[1:]:
        loudness = loudness * one(*cut)
    return loudness


def bell_draw(own_key, shape, spread, most, cuts=(), kind=jnp.bfloat16):
    values = spread * jax.random.normal(own_key, shape, jnp.float32)
    if cuts:
        values = values * levels(own_key, shape, cuts, -0.22, 0.18)
    return jnp.clip(values, -most, most).astype(kind)


def setup_inputs(seed: int = 0, part: int = 0) -> dict:
    splits = jax.random.split(jax.random.key(seed), 14)
    part_keys = jax.random.split(jax.random.fold_in(splits[13], part), 14)
    return {
        "hidden_states": bell_draw(part_keys[0], (HOOKS, TOKENS, HID), 1.0, 6.0, ((1, 16),)),
        "cell_of": draw_cell_of(jax.random.fold_in(splits[13], 71), part),
        "proj_four_weight": bell_draw(splits[2], (HID, C_FOUR), HID ** -0.5, 0.1875),
        "proj_four_bias": bell_draw(splits[3], (C_FOUR,), 0.5, 3.0, (), jnp.float32),
        "proj_two_weight": bell_draw(splits[4], (HID, C_TWO), HID ** -0.5, 0.1875),
        "proj_two_bias": bell_draw(splits[5], (C_TWO,), 0.5, 3.0, (), jnp.float32),
        "proj_same_weight": bell_draw(splits[6], (HID, C_SAME), HID ** -0.5, 0.1875),
        "proj_same_bias": bell_draw(splits[7], (C_SAME,), 0.5, 3.0, (), jnp.float32),
        "up4_weight": bell_draw(splits[8], (C_FOUR, 16 * C_FOUR), C_FOUR ** -0.5, 0.375),
        "up4_bias": bell_draw(splits[9], (C_FOUR,), 0.5, 3.0, (), jnp.float32),
        "up2_weight": bell_draw(splits[10], (C_TWO, 4 * C_TWO), C_TWO ** -0.5, 0.25),
        "up2_bias": bell_draw(splits[11], (C_TWO,), 0.5, 3.0, (), jnp.float32),
        "join_weight": bell_draw(splits[12], (3, 3, C_FOUR, FEAT), (9 * C_FOUR) ** -0.5, 0.125),
    }


def expand(proj, weight, bias_row, factor):
    height, columns, channels = proj.shape
    out_channels = weight.shape[1] // (factor * factor)
    flattened = jnp.dot(proj.reshape(-1, channels), weight, preferred_element_type=jnp.float32)
    flattened = flattened + jnp.tile(bias_row, factor * factor)[None, :]
    result = flattened.astype(jnp.bfloat16).reshape(height, columns, factor, factor, out_channels)
    return result.transpose(0, 2, 1, 3, 4).reshape(height * factor, columns * factor, out_channels)


def convolve(padded, weight, out_rows, out_cols):
    channels = padded.shape[2]
    total = jnp.zeros((out_rows, out_cols, weight.shape[3]), jnp.float32)
    for row_tap in range(3):
        for col_tap in range(3):
            window = padded[row_tap:row_tap + out_rows, col_tap:col_tap + out_cols]
            term = jnp.dot(window.reshape(-1, channels), weight[row_tap, col_tap], preferred_element_type=jnp.float32)
            total = total + term.reshape(out_rows, out_cols, -1)
    return total.astype(jnp.bfloat16)


def reference(hidden_states, cell_of, proj_four_weight, proj_four_bias, proj_two_weight, proj_two_bias, proj_same_weight, proj_same_bias, up4_weight, up4_bias, up2_weight, up2_bias, join_weight):
    grid_tokens = jnp.zeros(hidden_states.shape, jnp.bfloat16).at[:, cell_of, :].set(hidden_states)
    pairs = ((proj_four_weight, proj_four_bias), (proj_two_weight, proj_two_bias), (proj_same_weight, proj_same_bias))
    maps = []
    for hook in range(HOOKS):
        projected = jnp.dot(grid_tokens[hook], pairs[hook][0], preferred_element_type=jnp.float32) + pairs[hook][1]
        maps.append(projected.astype(jnp.bfloat16).reshape(GRID_H, GRID_W, -1))
    upsampled_four = expand(maps[0], up4_weight, up4_bias, 4)
    padded = jnp.pad(upsampled_four, ((1, 1), (1, 1), (0, 0)))
    joined_four = convolve(padded, join_weight, 4 * GRID_H, 4 * GRID_W)
    upsampled_two = expand(maps[1], up2_weight, up2_bias, 2)
    same_scale = maps[2]
    return (joined_four, upsampled_two, same_scale)
```

```python
import functools

import jax
import jax.numpy as jnp
from jax import lax
from jax.experimental import pallas as pl
from jax.experimental.pallas import tpu as pltpu
from jax.sharding import PartitionSpec as P

GRID_W = 64
MESH = pl.DeviceIdType.MESH


def partner(me, step):
    other = me
    bit = 1
    while bit <= step:
        if step & bit:
            other = other + bit * (1 - 2 * lax.rem(lax.div(me, bit), 2))
        bit *= 2
    return other


def dot(left, right):
    return jnp.dot(left, right, preferred_element_type=jnp.float32)


def kernel(
    shards,
    hid_hbm,
    table_hbm,
    w_four_hbm,
    b_four_hbm,
    w_two_hbm,
    b_two_hbm,
    w_same_hbm,
    b_same_hbm,
    up4_hbm,
    up4_b_hbm,
    up2_hbm,
    up2_b_hbm,
    join_hbm,
    joined_ref,
    two_ref,
    same_rows_ref,
    place_ref,
    hid,
    table,
    w_four,
    b_four,
    w_two,
    b_two,
    w_same,
    b_same,
    up4,
    up4_b,
    up2,
    up2_b,
    join,
    stage,
    send_four,
    send_two,
    send_same,
    recv_four,
    recv_two,
    recv_same,
    edge_out,
    edge_in,
    planes,
    joined_f32,
    two_f32,
    load_sem,
    send_sem,
    recv_sem,
    halo_send_sem,
    halo_recv_sem,
    relay_sem,
):
    me = lax.axis_index("rows")
    img = lax.axis_index("img")
    tok = hid.shape[1]
    per = tok // shards
    rows = tok // GRID_W
    group = shards // 4
    plane = lax.div(me, group)
    lower = plane < 2
    last = plane == 3
    beside = plane + 1 - 2 * lax.rem(plane, 2)

    names = (
        (table_hbm, table),
        (hid_hbm.at[0], hid.at[0]),
        (w_four_hbm, w_four),
        (b_four_hbm, b_four),
        (hid_hbm.at[1], hid.at[1]),
        (w_two_hbm, w_two),
        (b_two_hbm, b_two),
        (hid_hbm.at[2], hid.at[2]),
        (w_same_hbm, w_same),
        (b_same_hbm, b_same),
        (up4_hbm, up4),
        (up4_b_hbm, up4_b),
        (join_hbm, join),
        (up2_hbm, up2),
        (up2_b_hbm, up2_b),
    )
    loads = [pltpu.make_async_copy(src, dst, load_sem.at[i]) for i, (src, dst) in enumerate(names)]

    for load in loads[:10]:
        load.start()

    def row_in(other_plane, i):
        return partner(me, i) + (other_plane - plane) * group

    barrier = pltpu.get_barrier_semaphore()

    def greet(other_plane, some):
        for i in some:
            pl.semaphore_signal(barrier, inc=1, device_id=(img, row_in(other_plane, i)), device_id_type=MESH)

    @pl.when(~last)
    def _():
        greet(jnp.where(lower, 2, 0), range(group))
        greet(jnp.where(lower, 3, 1), range(group))
        greet(beside, range(group))

    greet(plane, range(1, group))

    loads[0].wait()
    mine = jnp.broadcast_to(table[pl.ds(me, 1), :].astype(jnp.float32), (tok, tok))
    smaller = (mine.T < mine).astype(jnp.float32)
    slot_row = jnp.sum(smaller, axis=0, keepdims=True)
    down = lax.broadcasted_iota(jnp.int32, (tok, tok), 0)
    across = lax.broadcasted_iota(jnp.int32, (tok, tok), 1)
    scatter = (down.astype(jnp.float32) == slot_row).astype(jnp.float32).astype(jnp.bfloat16)

    def project(hook, first, weight, bias, send):
        channels = weight.shape[1]
        for load in loads[first : first + 3]:
            load.wait()
        projected = (dot(hid[hook], weight[...]) + bias[...]).astype(jnp.bfloat16)
        stage[:, :channels] = dot(scatter, projected)
        if first == 1:
            for load in loads[10:]:
                load.start()
        for shard in range(shards):
            send[shard] = stage[shard * per : (shard + 1) * per, :channels].astype(jnp.bfloat16)

    def push(index, send, recv, other):
        pltpu.make_async_remote_copy(
            src_ref=send.at[other],
            dst_ref=recv.at[me],
            send_sem=send_sem.at[index],
            recv_sem=recv_sem.at[index, plane],
            device_id=(img, other),
            device_id_type=MESH,
        ).start()

    def exchange(index, send, recv, other_plane, some):
        for i in some:
            push(index, send, recv, row_in(other_plane, i))

    def exchange_early(index, send, recv):
        exchange(index, send, recv, jnp.where(lower, 2, 0), range(group))

        @pl.when(~lower)
        def _():
            exchange(index, send, recv, 1, range(group))

        @pl.when(plane != 2)
        def _():
            exchange(index, send, recv, beside, range(group))

        exchange(index, send, recv, plane, range(1, group))
        recv[me] = send[me]

    def bulk_wait(buffer, count, sem):
        part = buffer.at[pl.ds(0, count)]
        pltpu.make_async_copy(part, part, sem).wait()

    def arrive(index, recv, some):
        for other_plane in some:
            for mine in (False, True):

                @pl.when((plane == other_plane) == mine)
                def _():
                    bulk_wait(recv, group - mine, recv_sem.at[index, other_plane])

    def collect(index, recv):
        channels = recv.shape[2]
        for shard in range(shards):
            stage[shard * per : (shard + 1) * per, :channels] = recv[shard].astype(jnp.float32)
        return stage[:, :channels].astype(jnp.bfloat16)

    project(0, 1, w_four, b_four, send_four)
    pl.semaphore_wait(barrier, jnp.where(last, shards - 1, shards - 1 - group))

    @pl.when(last)
    def _():
        for other_plane in (0, 1, 2):
            to = row_in(other_plane, 0)
            pl.semaphore_signal(relay_sem, inc=1, device_id=(img, to), device_id_type=MESH)

    exchange_early(0, send_four, recv_four)
    project(1, 4, w_two, b_two, send_two)
    exchange_early(1, send_two, recv_two)
    project(2, 7, w_same, b_same, send_same)

    first_rows = range(group // 2)
    other_rows = range(group // 2, group)

    @pl.when(plane == 1)
    def _():
        exchange(2, send_same, recv_same, 2, first_rows)

    @pl.when(~last)
    def _():
        pl.semaphore_wait(relay_sem, 1)
        exchange(0, send_four, recv_four, 3, range(group))
        exchange(1, send_two, recv_two, 3, range(group))

    spot = lax.rem(me, group)
    faces_beside = jnp.where(lax.rem(plane, 2) == 0, spot == group - 1, spot == 0)
    faces_across = ((plane == 1) & (spot == group - 1)) | ((plane == 2) & (spot == 0))

    def exchange_same(after_halo, some):
        @pl.when((faces_across if after_halo else ~faces_across) & some)
        def _():
            exchange(2, send_same, recv_same, jnp.where(lower, 3, 0), range(group))

        @pl.when((faces_beside if after_halo else ~faces_beside) & some)
        def _():
            exchange(2, send_same, recv_same, beside, range(group))

        @pl.when((faces_across if after_halo else ~faces_across) & some)
        def _():
            exchange(2, send_same, recv_same, jnp.where(lower, 2, 1), other_rows)

            @pl.when(plane != 1)
            def _():
                exchange(2, send_same, recv_same, jnp.where(lower, 2, 1), first_rows)

    inner = (plane == 1) | (plane == 2)
    exchange_same(False, inner)
    exchange(2, send_same, recv_same, plane, range(1, group))
    recv_same[me] = send_same[me]

    wanted = down + me * tok
    source = jnp.zeros((tok, tok), jnp.float32)
    for shard in range(1, shards):
        source = source + jnp.where(table[shard : shard + 1, :] == wanted, float(shard), 0.0)
    source = jnp.broadcast_to(jnp.sum(source, axis=1, keepdims=True), (tok, tok))
    earlier = jnp.where((source == source.T) & (across < down), 1.0, 0.0)
    slot_col = source * per + jnp.sum(earlier, axis=1, keepdims=True)
    place = (across.astype(jnp.float32) == slot_col).astype(jnp.float32).astype(jnp.bfloat16)
    place_ref[...] = place

    arrive(0, recv_four, (3, 2))
    exchange_same(False, last)
    arrive(0, recv_four, (1, 0))
    exchange_same(False, plane == 0)
    tile_four = dot(place, collect(0, recv_four)).astype(jnp.bfloat16)
    edge_out[0] = tile_four[:GRID_W]
    edge_out[1] = tile_four[tok - GRID_W :]

    def halo(side):
        return pltpu.make_async_remote_copy(
            src_ref=edge_out.at[1 - side],
            dst_ref=edge_in.at[side],
            send_sem=halo_send_sem.at[side],
            recv_sem=halo_recv_sem.at[side],
            device_id=(img, me + 1 if side == 0 else me - 1),
            device_id_type=MESH,
        )

    has_below = me < shards - 1
    has_above = me > 0

    @pl.when(has_below)
    def _():
        halo(0).start()

    @pl.when(has_above)
    def _():
        halo(1).start()

    exchange_same(True, plane >= 0)

    column = lax.broadcasted_iota(jnp.int32, (GRID_W, 1), 0)
    c_up = join.shape[0] // 9

    def put_row(row, phase, values):
        where = pl.ds((row + 1) * GRID_W, GRID_W)
        planes[phase + 1, where, :] = values.astype(jnp.bfloat16)
        if phase == 3:
            moved = jnp.where(column == 0, 0.0, pltpu.roll(values, 1, axis=0))
            planes[0, where, :] = moved.astype(jnp.bfloat16)
        if phase == 0:
            moved = jnp.where(column == GRID_W - 1, 0.0, pltpu.roll(values, GRID_W - 1, axis=0))
            planes[5, where, :] = moved.astype(jnp.bfloat16)

    for load in loads[10:13]:
        load.wait()
    for a in range(4):
        for b in range(4):
            tap = a * 4 + b
            block = dot(tile_four, up4[:, tap * c_up : (tap + 1) * c_up]) + up4_b[...]
            for i in range(rows):
                put_row(4 * i + a, b, block[i * GRID_W : (i + 1) * GRID_W])

    half = joined_ref.shape[2] // 2

    def join_rows(phase, first, count):
        windows = [
            planes[phase + col, pl.ds((first + row) * GRID_W, count * GRID_W), :]
            for row in range(3)
            for col in range(3)
        ]
        total = dot(jnp.concatenate(windows, axis=1), join[...])
        for r in range(count):
            for h in range(2):
                joined_f32[first + r, h, pl.ds(phase, GRID_W, stride=4), :] = total[
                    r * GRID_W : (r + 1) * GRID_W, h * half : (h + 1) * half
                ]

    def finish_rows(first, count):
        for r in range(first, first + count):
            for h in range(2):
                joined_ref[r, :, h * half : (h + 1) * half] = joined_f32[r, h].astype(jnp.bfloat16)

    out_rows = 4 * rows
    for phase in range(4):
        join_rows(phase, 1, out_rows - 2)
    finish_rows(1, out_rows - 2)

    arrive(1, recv_two, range(4))
    tile_two = dot(place, collect(1, recv_two)).astype(jnp.bfloat16)
    for load in loads[13:]:
        load.wait()
    c_two = two_ref.shape[2]
    for a in range(2):
        for b in range(2):
            tap = a * 2 + b
            block = dot(tile_two, up2[:, tap * c_two : (tap + 1) * c_two]) + up2_b[...]
            for i in range(rows):
                for h in range(c_two // 128):
                    two_f32[2 * i + a, h, pl.ds(b, GRID_W, stride=2), :] = block[
                        i * GRID_W : (i + 1) * GRID_W, h * 128 : (h + 1) * 128
                    ]
    for r in range(2 * rows):
        for h in range(c_two // 128):
            two_ref[r, :, h * 128 : (h + 1) * 128] = two_f32[r, h].astype(jnp.bfloat16)

    @pl.when(has_below)
    def _():
        halo(0).wait_send()
        halo(1).wait_recv()

    @pl.when(has_above)
    def _():
        halo(1).wait_send()
        halo(0).wait_recv()

    for side, present, a, row in ((0, has_above, 3, -1), (1, has_below, 0, out_rows)):
        for b in range(4):
            tap = a * 4 + b
            block = dot(edge_in[side], up4[:, tap * c_up : (tap + 1) * c_up]) + up4_b[...]
            put_row(row, b, jnp.where(present, block, 0.0))
    for first in (0, out_rows - 1):
        for phase in range(4):
            join_rows(phase, first, 1)
        finish_rows(first, 1)

    arrive(2, recv_same, range(4))
    same_rows_ref[...] = collect(2, recv_same)

    for index, send in enumerate((send_four, send_two, send_same)):
        bulk_wait(send, shards - 1, send_sem.at[index])


def write_kernel(joined_ref, two_ref, same_rows_ref, place_ref, joined_out, two_out, same_out, same, sems):
    copies = [
        pltpu.make_async_copy(joined_ref, joined_out, sems.at[0]),
        pltpu.make_async_copy(two_ref, two_out, sems.at[1]),
        pltpu.make_async_copy(same, same_out, sems.at[2]),
    ]
    copies[0].start()
    copies[1].start()
    tile = dot(place_ref[...], same_rows_ref[...]).astype(jnp.bfloat16)
    for i in range(same.shape[0]):
        same[i] = tile[i * GRID_W : (i + 1) * GRID_W]
    copies[2].start()
    for copy in copies:
        copy.wait()


def body(
    hidden_states,
    cell_of,
    proj_four_weight,
    proj_four_bias,
    proj_two_weight,
    proj_two_bias,
    proj_same_weight,
    proj_same_bias,
    up4_weight,
    up4_bias,
    up2_weight,
    up2_bias,
    join_weight,
):
    tok = hidden_states.shape[1]
    shards = lax.axis_size("rows")
    per = tok // shards
    rows = tok // GRID_W
    operands = (
        hidden_states,
        cell_of.reshape(shards, tok),
        proj_four_weight,
        proj_four_bias[None, :],
        proj_two_weight,
        proj_two_bias[None, :],
        proj_same_weight,
        proj_same_bias[None, :],
        up4_weight,
        up4_bias[None, :],
        up2_weight,
        up2_bias[None, :],
        join_weight.reshape(-1, join_weight.shape[3]),
    )
    c_four = proj_four_weight.shape[1]
    c_two = proj_two_weight.shape[1]
    c_same = proj_same_weight.shape[1]
    feat = join_weight.shape[3]
    widths = (c_four, c_two, c_same)
    wire = [pltpu.VMEM((shards, per, c), jnp.bfloat16) for c in widths]
    scratch = [pltpu.VMEM(x.shape, x.dtype) for x in operands]
    scratch += [pltpu.VMEM((tok, max(widths)), jnp.float32)]
    scratch += wire + wire
    scratch += [
        pltpu.VMEM((2, GRID_W, c_four), jnp.bfloat16),
        pltpu.VMEM((2, GRID_W, c_four), jnp.bfloat16),
        pltpu.VMEM((6, (4 * rows + 2) * GRID_W, c_four), jnp.bfloat16),
        pltpu.VMEM((4 * rows, 2, 4 * GRID_W, feat // 2), jnp.float32),
        pltpu.VMEM((2 * rows, c_two // 128, 2 * GRID_W, 128), jnp.float32),
        pltpu.SemaphoreType.DMA((15,)),
        pltpu.SemaphoreType.DMA((3,)),
        pltpu.SemaphoreType.DMA((3, 4)),
        pltpu.SemaphoreType.DMA((2,)),
        pltpu.SemaphoreType.DMA((2,)),
        pltpu.SemaphoreType.REGULAR,
    ]
    operands = tuple(pltpu.with_memory_space_constraint(x, pltpu.HBM) for x in operands)
    results = pl.pallas_call(
        functools.partial(kernel, shards),
        out_shape=(
            pltpu.VMEM((4 * rows, 4 * GRID_W, feat), jnp.bfloat16),
            pltpu.VMEM((2 * rows, 2 * GRID_W, c_two), jnp.bfloat16),
            pltpu.VMEM((tok, c_same), jnp.bfloat16),
            pltpu.VMEM((tok, tok), jnp.bfloat16),
        ),
        in_specs=[pl.BlockSpec(memory_space=pl.ANY)] * len(operands),
        out_specs=(pl.BlockSpec(memory_space=pltpu.VMEM),) * 4,
        scratch_shapes=scratch,
        compiler_params=pltpu.CompilerParams(
            collective_id=0, has_side_effects=True, vmem_limit_bytes=40 * 1024 * 1024
        ),
    )(*operands)
    results = tuple(pltpu.with_memory_space_constraint(x, pltpu.VMEM) for x in results)
    return pl.pallas_call(
        write_kernel,
        out_shape=(
            jax.ShapeDtypeStruct((4 * rows, 4 * GRID_W, feat), jnp.bfloat16),
            jax.ShapeDtypeStruct((2 * rows, 2 * GRID_W, c_two), jnp.bfloat16),
            jax.ShapeDtypeStruct((rows, GRID_W, c_same), jnp.bfloat16),
        ),
        in_specs=[pl.BlockSpec(memory_space=pltpu.VMEM)] * 4,
        out_specs=(pl.BlockSpec(memory_space=pl.ANY),) * 3,
        scratch_shapes=[
            pltpu.VMEM((rows, GRID_W, c_same), jnp.bfloat16),
            pltpu.SemaphoreType.DMA((3,)),
        ],
        compiler_params=pltpu.CompilerParams(vmem_limit_bytes=8 * 1024 * 1024),
    )(*results)


def solution(mesh):
    rows = P(("img", "rows"), None, None)
    return jax.shard_map(
        body,
        mesh=mesh,
        in_specs=(P(None, ("img", "rows"), None),) + (P(),) * 12,
        out_specs=(rows, rows, rows),
        check_vma=False,
    )
```

```python
import functools

import jax
import jax.numpy as jnp
from jax import lax
from jax.experimental import pallas as pl
from jax.experimental.pallas import tpu as pltpu
from jax.sharding import PartitionSpec as P

GRID_W = 64
MESH = pl.DeviceIdType.MESH


def partner(me, step):
    other = me
    bit = 1
    while bit <= step:
        if step & bit:
            other = other + bit * (1 - 2 * lax.rem(lax.div(me, bit), 2))
        bit *= 2
    return other


def dot(left, right):
    return jnp.dot(left, right, preferred_element_type=jnp.float32)


def kernel(
    shards,
    hid_hbm,
    table_hbm,
    w_four_hbm,
    b_four_hbm,
    w_two_hbm,
    b_two_hbm,
    w_same_hbm,
    b_same_hbm,
    up4_hbm,
    up4_b_hbm,
    up2_hbm,
    up2_b_hbm,
    join_hbm,
    joined_ref,
    two_ref,
    same_rows_ref,
    place_ref,
    hid,
    table,
    w_four,
    b_four,
    w_two,
    b_two,
    w_same,
    b_same,
    up4,
    up4_b,
    up2,
    up2_b,
    join,
    stage,
    send_four,
    send_two,
    send_same,
    recv_four,
    recv_two,
    recv_spare,
    edge_out,
    edge_in,
    planes,
    joined_f32,
    two_f32,
    load_sem,
    send_sem,
    recv_sem,
    halo_send_sem,
    halo_recv_sem,
    relay_sem,
):
    me = lax.axis_index("rows")
    img = lax.axis_index("img")
    tok = hid.shape[1]
    per = tok // shards
    rows = tok // GRID_W
    block = send_four.shape[1]
    split = block // per
    direct = block == 16
    recv_same = same_rows_ref if direct else recv_spare
    group = shards // 4
    plane = lax.div(me, group)
    lower = plane < 2
    last = plane == 3
    beside = plane + 1 - 2 * lax.rem(plane, 2)

    names = (
        (table_hbm, table),
        (hid_hbm.at[0], hid.at[0]),
        (w_four_hbm, w_four),
        (b_four_hbm, b_four),
        (hid_hbm.at[1], hid.at[1]),
        (w_two_hbm, w_two),
        (b_two_hbm, b_two),
        (hid_hbm.at[2], hid.at[2]),
        (w_same_hbm, w_same),
        (b_same_hbm, b_same),
        (up4_hbm, up4),
        (up4_b_hbm, up4_b),
        (join_hbm, join),
        (up2_hbm, up2),
        (up2_b_hbm, up2_b),
    )
    stages = (0, 1, 1, 1, 2, 2, 2, 3, 3, 3, 4, 4, 4, 5, 5)
    loads = [pltpu.make_async_copy(src, dst, load_sem.at[stage_of]) for (src, dst), stage_of in zip(names, stages)]

    for load in loads[:10]:
        load.start()

    def row_in(other_plane, i):
        return partner(me, i) + (other_plane - plane) * group

    barrier = pltpu.get_barrier_semaphore()

    def greet(other_plane, some):
        for i in some:
            pl.semaphore_signal(barrier, inc=1, device_id=(img, row_in(other_plane, i)), device_id_type=MESH)

    @pl.when(~last)
    def _():
        greet(jnp.where(lower, 2, 0), range(group))
        greet(jnp.where(lower, 3, 1), range(group))
        greet(beside, range(group))

    greet(plane, range(1, group))

    loads[0].wait()
    mine = jnp.broadcast_to(table[pl.ds(me, 1), :].astype(jnp.float32), (tok, tok))
    smaller = (mine.T < mine).astype(jnp.float32)
    slot_row = jnp.sum(smaller, axis=0, keepdims=True)
    down = lax.broadcasted_iota(jnp.int32, (tok, tok), 0)
    across = lax.broadcasted_iota(jnp.int32, (tok, tok), 1)
    shard_row = lax.div(table[pl.ds(me, 1), :], tok).astype(jnp.float32)
    packed_row = slot_row + shard_row * (block - per)
    packed_row = jnp.concatenate([packed_row + part * per for part in range(split)], axis=1)
    packed = lax.broadcasted_iota(jnp.int32, (shards * block, split * tok), 0).astype(jnp.float32)
    scatter = (packed == packed_row).astype(jnp.float32).astype(jnp.bfloat16)

    def project(hook, first, weight, bias, send):
        channels = weight.shape[1]
        for load in loads[first : first + 3]:
            load.wait()
        projected = (dot(hid[hook], weight[...]) + bias[...]).astype(jnp.bfloat16)
        width = channels // split
        stacked = [projected[:, part * width : (part + 1) * width] for part in range(split)]
        ordered = dot(scatter, jnp.concatenate(stacked, axis=0))
        if first == 1:
            for load in loads[10:]:
                load.start()
        if direct:
            send[...] = ordered.astype(jnp.bfloat16).reshape(send.shape)
        else:
            stage[:, :channels] = ordered
            for shard in range(shards):
                send[shard] = stage[shard * per : (shard + 1) * per, :channels].astype(jnp.bfloat16)

    def push(index, send, recv, other):
        pltpu.make_async_remote_copy(
            src_ref=send.at[other],
            dst_ref=recv.at[me],
            send_sem=send_sem,
            recv_sem=recv_sem.at[jnp.where(lower, 0, 1) if index == 0 else index + 1],
            device_id=(img, other),
            device_id_type=MESH,
        ).start()

    def exchange(index, send, recv, other_plane, some):
        for i in reversed(some):
            push(index, send, recv, row_in(other_plane, i))

    def exchange_early(index, send, recv):
        @pl.when(~lower)
        def _():
            exchange(index, send, recv, 1, range(group))

        exchange(index, send, recv, jnp.where(lower, 2, 0), range(group))

        @pl.when(plane != 2)
        def _():
            exchange(index, send, recv, beside, range(group))

        exchange(index, send, recv, plane, range(1, group))
        recv[me] = send[me]

    def bulk_wait(buffer, count, sem):
        part = buffer.at[pl.ds(0, count)]
        pltpu.make_async_copy(part, part, sem).wait()

    def arrive(recv, planes_in, own, sem):
        for mine in (0, 1):

            @pl.when(own == (mine == 1))
            def _():
                bulk_wait(recv, planes_in * group - mine, recv_sem.at[sem])

    def collect(recv):
        width = recv.shape[2]
        if direct:
            return recv[...].reshape(shards * block, width)
        for shard in range(shards):
            stage[shard * per : (shard + 1) * per, :width] = recv[shard].astype(jnp.float32)
        return stage[:, :width].astype(jnp.bfloat16)

    def in_cells(recv):
        tile = dot(place, collect(recv)).astype(jnp.bfloat16)
        return jnp.concatenate([tile[part * tok : (part + 1) * tok] for part in range(split)], axis=1)

    project(0, 1, w_four, b_four, send_four)
    pl.semaphore_wait(barrier, jnp.where(last, shards - 1, shards - 1 - group))

    @pl.when(last)
    def _():
        for other_plane in (0, 1, 2):
            to = row_in(other_plane, 0)
            pl.semaphore_signal(relay_sem, inc=1, device_id=(img, to), device_id_type=MESH)

    exchange_early(0, send_four, recv_four)
    project(1, 4, w_two, b_two, send_two)
    exchange_early(1, send_two, recv_two)
    project(2, 7, w_same, b_same, send_same)

    other_rows = range(group // 2)
    first_rows = range(group // 2, group)

    @pl.when(plane == 1)
    def _():
        exchange(2, send_same, recv_same, 2, first_rows)

    @pl.when(~last)
    def _():
        pl.semaphore_wait(relay_sem, 1)
        exchange(0, send_four, recv_four, 3, range(group))
        exchange(1, send_two, recv_two, 3, range(group))

    spot = lax.rem(me, group)
    faces_beside = jnp.where(lax.rem(plane, 2) == 0, spot == group - 1, spot == 0)
    faces_across = ((plane == 1) & (spot == group - 1)) | ((plane == 2) & (spot == 0))

    inner = (plane == 1) | (plane == 2)

    def exchange_same(after_halo, some):
        if not after_halo:

            @pl.when(some)
            def _():
                exchange(2, send_same, recv_same, jnp.where(lower, 3, 0), range(group))

        @pl.when((faces_beside if after_halo else ~faces_beside) & some)
        def _():
            exchange(2, send_same, recv_same, beside, range(group))

        @pl.when((inner if after_halo else ~inner) & some)
        def _():
            exchange(2, send_same, recv_same, jnp.where(lower, 2, 1), other_rows)

            @pl.when(plane != 1)
            def _():
                exchange(2, send_same, recv_same, jnp.where(lower, 2, 1), first_rows)

    exchange_same(False, inner)
    exchange(2, send_same, recv_same, plane, range(1, group))
    recv_same[me] = send_same[me]

    wanted = down + me * tok
    source = jnp.zeros((tok, tok), jnp.float32)
    for shard in range(1, shards):
        source = source + jnp.where(table[shard : shard + 1, :] == wanted, float(shard), 0.0)
    source = jnp.broadcast_to(jnp.sum(source, axis=1, keepdims=True), (tok, tok))
    earlier = jnp.where((source == source.T) & (across < down), 1.0, 0.0)
    slot_col = source[:, :1] * block + jnp.sum(earlier, axis=1, keepdims=True)
    slot_col = jnp.concatenate([slot_col + part * per for part in range(split)], axis=0)
    packed = lax.broadcasted_iota(jnp.int32, (split * tok, shards * block), 1).astype(jnp.float32)
    place = (packed == slot_col).astype(jnp.float32).astype(jnp.bfloat16)
    place_ref[...] = place

    arrive(recv_four, 2, ~lower, 1)
    exchange_same(False, last)
    arrive(recv_four, 2, lower, 0)
    exchange_same(False, plane == 0)
    tile_four = in_cells(recv_four)
    edge_out[0] = tile_four[:GRID_W]
    edge_out[1] = tile_four[tok - GRID_W :]

    def halo(side):
        return pltpu.make_async_remote_copy(
            src_ref=edge_out.at[1 - side],
            dst_ref=edge_in.at[side],
            send_sem=halo_send_sem,
            recv_sem=halo_recv_sem.at[side],
            device_id=(img, me + 1 if side == 0 else me - 1),
            device_id_type=MESH,
        )

    has_below = me < shards - 1
    has_above = me > 0

    @pl.when(has_below)
    def _():
        halo(0).start()

    @pl.when(has_above)
    def _():
        halo(1).start()

    exchange_same(True, plane >= 0)

    column = lax.broadcasted_iota(jnp.int32, (GRID_W, 1), 0)
    c_up = join.shape[0] // 9

    def put_row(row, phase, values):
        where = pl.ds((row + 1) * GRID_W, GRID_W)
        planes[phase + 1, where, :] = values.astype(jnp.bfloat16)
        if phase == 3:
            moved = jnp.where(column == 0, 0.0, pltpu.roll(values, 1, axis=0))
            planes[0, where, :] = moved.astype(jnp.bfloat16)
        if phase == 0:
            moved = jnp.where(column == GRID_W - 1, 0.0, pltpu.roll(values, GRID_W - 1, axis=0))
            planes[5, where, :] = moved.astype(jnp.bfloat16)

    for load in loads[10:13]:
        load.wait()
    for a in range(4):
        for b in range(4):
            tap = a * 4 + b
            value = dot(tile_four, up4[:, tap * c_up : (tap + 1) * c_up]) + up4_b[...]
            for i in range(rows):
                put_row(4 * i + a, b, value[i * GRID_W : (i + 1) * GRID_W])

    half = joined_ref.shape[2] // 2

    def join_rows(jobs, count):
        windows = [
            jnp.concatenate(
                [
                    planes[phase + col, pl.ds((first + row) * GRID_W, count * GRID_W), :]
                    for row in range(3)
                    for col in range(3)
                ],
                axis=1,
            )
            for phase, first in jobs
        ]
        total = dot(jnp.concatenate(windows, axis=0), join[...])
        for job, (phase, first) in enumerate(jobs):
            for r in range(count):
                at = (job * count + r) * GRID_W
                for h in range(2):
                    joined_f32[first + r, h, pl.ds(phase, GRID_W, stride=4), :] = total[
                        at : at + GRID_W, h * half : (h + 1) * half
                    ]

    def finish_rows(first, count):
        for r in range(first, first + count):
            for h in range(2):
                joined_ref[r, :, h * half : (h + 1) * half] = joined_f32[r, h].astype(jnp.bfloat16)

    out_rows = 4 * rows
    for phase in range(4):
        join_rows([(phase, 1)], out_rows - 2)
    finish_rows(1, out_rows - 2)

    bulk_wait(recv_two, shards - 1, recv_sem.at[2])
    tile_two = in_cells(recv_two)
    for load in loads[13:]:
        load.wait()
    c_two = two_ref.shape[2]
    for a in range(2):
        for b in range(2):
            tap = a * 2 + b
            value = dot(tile_two, up2[:, tap * c_two : (tap + 1) * c_two]) + up2_b[...]
            for i in range(rows):
                for h in range(c_two // 128):
                    two_f32[2 * i + a, h, pl.ds(b, GRID_W, stride=2), :] = value[
                        i * GRID_W : (i + 1) * GRID_W, h * 128 : (h + 1) * 128
                    ]
    for r in range(2 * rows):
        for h in range(c_two // 128):
            two_ref[r, :, h * 128 : (h + 1) * 128] = two_f32[r, h].astype(jnp.bfloat16)

    @pl.when(has_below)
    def _():
        halo(0).wait_send()
        halo(1).wait_recv()

    @pl.when(has_above)
    def _():
        halo(1).wait_send()
        halo(0).wait_recv()

    for side, present, a, row in ((0, has_above, 3, -1), (1, has_below, 0, out_rows)):
        for b in range(4):
            tap = a * 4 + b
            value = dot(edge_in[side], up4[:, tap * c_up : (tap + 1) * c_up]) + up4_b[...]
            put_row(row, b, jnp.where(present, value, 0.0))
    join_rows([(phase, first) for first in (0, out_rows - 1) for phase in range(4)], 1)
    finish_rows(0, 1)
    finish_rows(out_rows - 1, 1)

    bulk_wait(recv_same, shards - 1, recv_sem.at[3])
    if not direct:
        same_rows_ref[...] = collect(recv_same)

    for send in (send_four, send_two, send_same):
        bulk_wait(send, shards - 1, send_sem)


def write_kernel(joined_ref, two_ref, same_rows_ref, place_ref, joined_out, two_out, same_out, same, sem):
    copies = [
        pltpu.make_async_copy(src.at[pl.ds(i, 1)], dst.at[pl.ds(i, 1)], sem)
        for src, dst in ((joined_ref, joined_out), (two_ref, two_out))
        for i in range(src.shape[0])
    ]
    for copy in copies:
        copy.start()
    arrived = same_rows_ref[...]
    width = arrived.shape[-1]
    tile = dot(place_ref[...], arrived.reshape(-1, width)).astype(jnp.bfloat16)
    tok = same.shape[0] * GRID_W
    for part in range(same.shape[2] // width):
        for i in range(same.shape[0]):
            at = part * tok + i * GRID_W
            same[i, :, part * width : (part + 1) * width] = tile[at : at + GRID_W]
    copies.append(pltpu.make_async_copy(same, same_out, sem))
    copies[-1].start()
    for copy in copies:
        copy.wait()


def body(
    hidden_states,
    cell_of,
    proj_four_weight,
    proj_four_bias,
    proj_two_weight,
    proj_two_bias,
    proj_same_weight,
    proj_same_bias,
    up4_weight,
    up4_bias,
    up2_weight,
    up2_bias,
    join_weight,
):
    tok = hidden_states.shape[1]
    shards = lax.axis_size("rows")
    per = tok // shards
    rows = tok // GRID_W
    operands = (
        hidden_states,
        cell_of.reshape(shards, tok),
        proj_four_weight,
        proj_four_bias[None, :],
        proj_two_weight,
        proj_two_bias[None, :],
        proj_same_weight,
        proj_same_bias[None, :],
        up4_weight,
        up4_bias[None, :],
        up2_weight,
        up2_bias[None, :],
        join_weight.reshape(-1, join_weight.shape[3]),
    )
    c_four = proj_four_weight.shape[1]
    c_two = proj_two_weight.shape[1]
    c_same = proj_same_weight.shape[1]
    feat = join_weight.shape[3]
    widths = (c_four, c_two, c_same)
    direct = 16 % per == 0 and all(c * per % (16 * 128) == 0 for c in widths)
    block = 16 if direct else per
    split = block // per
    wire = [pltpu.VMEM((shards, block, c // split), jnp.bfloat16) for c in widths]
    spare = pltpu.VMEM((8, 128), jnp.bfloat16) if direct else wire[2]
    arrived = wire[2].shape if direct else (tok, c_same)
    scratch = [pltpu.VMEM(x.shape, x.dtype) for x in operands]
    scratch += [pltpu.VMEM((tok, max(widths)), jnp.float32)]
    scratch += wire + wire[:2] + [spare]
    scratch += [
        pltpu.VMEM((2, GRID_W, c_four), jnp.bfloat16),
        pltpu.VMEM((2, GRID_W, c_four), jnp.bfloat16),
        pltpu.VMEM((6, (4 * rows + 2) * GRID_W, c_four), jnp.bfloat16),
        pltpu.VMEM((4 * rows, 2, 4 * GRID_W, feat // 2), jnp.float32),
        pltpu.VMEM((2 * rows, c_two // 128, 2 * GRID_W, 128), jnp.float32),
        pltpu.SemaphoreType.DMA((6,)),
        pltpu.SemaphoreType.DMA,
        pltpu.SemaphoreType.DMA((4,)),
        pltpu.SemaphoreType.DMA,
        pltpu.SemaphoreType.DMA((2,)),
        pltpu.SemaphoreType.REGULAR,
    ]
    operands = tuple(pltpu.with_memory_space_constraint(x, pltpu.HBM) for x in operands)
    results = pl.pallas_call(
        functools.partial(kernel, shards),
        out_shape=(
            pltpu.VMEM((4 * rows, 4 * GRID_W, feat), jnp.bfloat16),
            pltpu.VMEM((2 * rows, 2 * GRID_W, c_two), jnp.bfloat16),
            pltpu.VMEM(arrived, jnp.bfloat16),
            pltpu.VMEM((split * tok, shards * block), jnp.bfloat16),
        ),
        in_specs=[pl.BlockSpec(memory_space=pl.ANY)] * len(operands),
        out_specs=(pl.BlockSpec(memory_space=pltpu.VMEM),) * 4,
        scratch_shapes=scratch,
        compiler_params=pltpu.CompilerParams(
            collective_id=0, has_side_effects=True, vmem_limit_bytes=40 * 1024 * 1024
        ),
    )(*operands)
    results = tuple(pltpu.with_memory_space_constraint(x, pltpu.VMEM) for x in results)
    return pl.pallas_call(
        write_kernel,
        out_shape=(
            jax.ShapeDtypeStruct((4 * rows, 4 * GRID_W, feat), jnp.bfloat16),
            jax.ShapeDtypeStruct((2 * rows, 2 * GRID_W, c_two), jnp.bfloat16),
            jax.ShapeDtypeStruct((rows, GRID_W, c_same), jnp.bfloat16),
        ),
        in_specs=[pl.BlockSpec(memory_space=pltpu.VMEM)] * 4,
        out_specs=(pl.BlockSpec(memory_space=pl.ANY),) * 3,
        scratch_shapes=[
            pltpu.VMEM((rows, GRID_W, c_same), jnp.bfloat16),
            pltpu.SemaphoreType.DMA,
        ],
        compiler_params=pltpu.CompilerParams(vmem_limit_bytes=8 * 1024 * 1024),
    )(*results)


def solution(mesh):
    rows = P(("img", "rows"), None, None)
    return jax.shard_map(
        body,
        mesh=mesh,
        in_specs=(P(None, ("img", "rows"), None),) + (P(),) * 12,
        out_specs=(rows, rows, rows),
        check_vma=False,
    )
```

```python
import functools

import jax
import jax.numpy as jnp
from jax import lax
from jax.experimental import pallas as pl
from jax.experimental.pallas import tpu as pltpu
from jax.sharding import PartitionSpec as P

GRID_W = 64
MESH = pl.DeviceIdType.MESH


def partner(me, step):
    other = me
    bit = 1
    while bit <= step:
        if step & bit:
            other = other + bit * (1 - 2 * lax.rem(lax.div(me, bit), 2))
        bit *= 2
    return other


def dot(left, right):
    return jnp.dot(left, right, preferred_element_type=jnp.float32)


def kernel(
    shards,
    hid_hbm,
    table_hbm,
    w_four_hbm,
    b_four_hbm,
    w_two_hbm,
    b_two_hbm,
    w_same_hbm,
    b_same_hbm,
    up4_hbm,
    up4_b_hbm,
    up2_hbm,
    up2_b_hbm,
    join_hbm,
    joined_ref,
    two_ref,
    same_rows_ref,
    place_ref,
    hid,
    table,
    w_four,
    b_four,
    w_two,
    b_two,
    w_same,
    b_same,
    up4,
    up4_b,
    up2,
    up2_b,
    join,
    stage,
    send_four,
    send_two,
    send_same,
    recv_four,
    recv_two,
    recv_spare,
    edge_out,
    edge_in,
    planes,
    joined_f32,
    two_f32,
    load_sem,
    send_sem,
    recv_sem,
    halo_send_sem,
    halo_recv_sem,
    relay_sem,
):
    me = lax.axis_index("rows")
    img = lax.axis_index("img")
    tok = hid.shape[1]
    per = tok // shards
    rows = tok // GRID_W
    block = send_four.shape[1]
    split = block // per
    direct = block == 16
    recv_same = same_rows_ref if direct else recv_spare
    group = shards // 4
    plane = lax.div(me, group)
    lower = plane < 2
    last = plane == 3
    beside = plane + 1 - 2 * lax.rem(plane, 2)

    names = (
        (table_hbm, table),
        (hid_hbm.at[0], hid.at[0]),
        (w_four_hbm, w_four),
        (b_four_hbm, b_four),
        (hid_hbm.at[1], hid.at[1]),
        (w_two_hbm, w_two),
        (b_two_hbm, b_two),
        (hid_hbm.at[2], hid.at[2]),
        (w_same_hbm, w_same),
        (b_same_hbm, b_same),
        (up4_hbm, up4),
        (up4_b_hbm, up4_b),
        (join_hbm, join),
        (up2_hbm, up2),
        (up2_b_hbm, up2_b),
    )
    stages = (0, 1, 1, 1, 2, 2, 2, 3, 3, 3, 4, 4, 4, 4, 4)
    loads = [pltpu.make_async_copy(src, dst, load_sem.at[stage_of]) for (src, dst), stage_of in zip(names, stages)]

    for load in loads[:4]:
        load.start()

    def row_in(other_plane, i):
        return partner(me, i) + (other_plane - plane) * group

    barrier = pltpu.get_barrier_semaphore()

    def greet(other_plane, some):
        for i in some:
            pl.semaphore_signal(barrier, inc=1, device_id=(img, row_in(other_plane, i)), device_id_type=MESH)

    @pl.when(~last)
    def _():
        greet(jnp.where(lower, 2, 0), range(group))
        greet(jnp.where(lower, 3, 1), range(group))
        greet(beside, range(group))

    greet(plane, range(1, group))

    for load in loads[4:10]:
        load.start()

    loads[0].wait()
    mine = jnp.broadcast_to(table[pl.ds(me, 1), :].astype(jnp.float32), (tok, tok))
    smaller = (mine.T < mine).astype(jnp.float32)
    slot_row = jnp.sum(smaller, axis=0, keepdims=True)
    down = lax.broadcasted_iota(jnp.int32, (tok, tok), 0)
    across = lax.broadcasted_iota(jnp.int32, (tok, tok), 1)
    shard_row = lax.div(table[pl.ds(me, 1), :], tok).astype(jnp.float32)
    packed_row = slot_row + shard_row * (block - per)
    packed_row = jnp.concatenate([packed_row + part * per for part in range(split)], axis=1)
    packed = lax.broadcasted_iota(jnp.int32, (shards * block, split * tok), 0).astype(jnp.float32)
    scatter = (packed == packed_row).astype(jnp.float32).astype(jnp.bfloat16)

    def project(hook, first, weight, bias, send):
        channels = weight.shape[1]
        for load in loads[first : first + 3]:
            load.wait()
        projected = (dot(hid[hook], weight[...]) + bias[...]).astype(jnp.bfloat16)
        width = channels // split
        stacked = [projected[:, part * width : (part + 1) * width] for part in range(split)]
        ordered = dot(scatter, jnp.concatenate(stacked, axis=0))
        if first == 1:
            for load in loads[10:]:
                load.start()
        if direct:
            send[...] = ordered.astype(jnp.bfloat16).reshape(send.shape)
        else:
            stage[:, :channels] = ordered
            for shard in range(shards):
                send[shard] = stage[shard * per : (shard + 1) * per, :channels].astype(jnp.bfloat16)

    def push(index, send, recv, other):
        pltpu.make_async_remote_copy(
            src_ref=send.at[other],
            dst_ref=recv.at[me],
            send_sem=send_sem,
            recv_sem=recv_sem.at[jnp.where(lower, 0, 1) if index == 0 else index + 1],
            device_id=(img, other),
            device_id_type=MESH,
        ).start()

    def exchange(index, send, recv, other_plane, some):
        for i in reversed(some):
            push(index, send, recv, row_in(other_plane, i))

    def exchange_early(index, send, recv):
        exchange(index, send, recv, jnp.where(lower, 2, 0), range(group))

        @pl.when(~lower)
        def _():
            exchange(index, send, recv, 1, range(group))

        @pl.when(plane != 2)
        def _():
            exchange(index, send, recv, beside, range(group))

        exchange(index, send, recv, plane, range(1, group))
        recv[me] = send[me]

    def bulk_wait(buffer, count, sem):
        part = buffer.at[pl.ds(0, count)]
        pltpu.make_async_copy(part, part, sem).wait()

    def arrive(recv, planes_in, own, sem):
        for mine in (0, 1):

            @pl.when(own == (mine == 1))
            def _():
                bulk_wait(recv, planes_in * group - mine, recv_sem.at[sem])

    def collect(recv):
        width = recv.shape[2]
        if direct:
            return recv[...].reshape(shards * block, width)
        for shard in range(shards):
            stage[shard * per : (shard + 1) * per, :width] = recv[shard].astype(jnp.float32)
        return stage[:, :width].astype(jnp.bfloat16)

    def in_cells(recv):
        tile = dot(place, collect(recv)).astype(jnp.bfloat16)
        return jnp.concatenate([tile[part * tok : (part + 1) * tok] for part in range(split)], axis=1)

    project(0, 1, w_four, b_four, send_four)

    @pl.when(plane >= 2)
    def _():
        pl.semaphore_wait(barrier, jnp.where(last, shards - 1, shards - 1 - group))

        @pl.when(last)
        def _():
            for other_plane in (0, 1, 2):
                to = row_in(other_plane, 0)
                pl.semaphore_signal(relay_sem, inc=1, device_id=(img, to), device_id_type=MESH)

        exchange_early(0, send_four, recv_four)

    project(1, 4, w_two, b_two, send_two)

    @pl.when(plane == 1)
    def _():
        pl.semaphore_wait(barrier, shards - 1 - group)
        exchange_early(0, send_four, recv_four)

    @pl.when(plane > 0)
    def _():
        exchange_early(1, send_two, recv_two)

    project(2, 7, w_same, b_same, send_same)

    @pl.when(plane == 0)
    def _():
        pl.semaphore_wait(barrier, shards - 1 - group)
        exchange_early(0, send_four, recv_four)
        exchange_early(1, send_two, recv_two)

    other_rows = range(group // 2)
    first_rows = range(group // 2, group)

    @pl.when(plane == 1)
    def _():
        exchange(2, send_same, recv_same, 2, first_rows)

    @pl.when(~last)
    def _():
        pl.semaphore_wait(relay_sem, 1)
        exchange(0, send_four, recv_four, 3, range(group))
        exchange(1, send_two, recv_two, 3, range(group))

    spot = lax.rem(me, group)
    faces_beside = jnp.where(lax.rem(plane, 2) == 0, spot == group - 1, spot == 0)

    inner = (plane == 1) | (plane == 2)
    outer = ~inner
    faces_across = ((plane == 1) & (spot == group - 1)) | ((plane == 2) & (spot == 0))

    def same_far(some, rows_to=range(group)):
        @pl.when(some)
        def _():
            exchange(2, send_same, recv_same, jnp.where(lower, 3, 0), rows_to)

    def same_beside(some):
        @pl.when(some)
        def _():
            exchange(2, send_same, recv_same, beside, range(group))

    def same_across(some):
        @pl.when(some & (plane != 1))
        def _():
            exchange(2, send_same, recv_same, jnp.where(lower, 2, 1), first_rows)

        @pl.when(some)
        def _():
            exchange(2, send_same, recv_same, jnp.where(lower, 2, 1), other_rows)

    same_far(inner)
    same_beside(inner)
    exchange(2, send_same, recv_same, plane, range(1, group))
    recv_same[me] = send_same[me]

    wanted = down + me * tok
    source = jnp.zeros((tok, tok), jnp.float32)
    for shard in range(1, shards):
        source = source + jnp.where(table[shard : shard + 1, :] == wanted, float(shard), 0.0)
    source = jnp.broadcast_to(jnp.sum(source, axis=1, keepdims=True), (tok, tok))
    earlier = jnp.where((source == source.T) & (across < down), 1.0, 0.0)
    slot_col = source[:, :1] * block + jnp.sum(earlier, axis=1, keepdims=True)
    slot_col = jnp.concatenate([slot_col + part * per for part in range(split)], axis=0)
    packed = lax.broadcasted_iota(jnp.int32, (split * tok, shards * block), 1).astype(jnp.float32)
    place = (packed == slot_col).astype(jnp.float32).astype(jnp.bfloat16)
    place_ref[...] = place

    arrive(recv_four, 2, ~lower, 1)
    same_far(last)
    same_beside(last & ~faces_beside)
    same_across(last)
    arrive(recv_four, 2, lower, 0)
    free = (plane == 0) & ~faces_beside
    same_far(free)
    same_beside(free)
    same_across(free)
    tile_four = in_cells(recv_four)
    edge_out[0] = tile_four[:GRID_W]
    edge_out[1] = tile_four[tok - GRID_W :]

    def halo(side):
        return pltpu.make_async_remote_copy(
            src_ref=edge_out.at[1 - side],
            dst_ref=edge_in.at[side],
            send_sem=halo_send_sem,
            recv_sem=halo_recv_sem.at[side],
            device_id=(img, me + 1 if side == 0 else me - 1),
            device_id_type=MESH,
        )

    has_below = me < shards - 1
    has_above = me > 0

    @pl.when(has_below)
    def _():
        halo(0).start()

    @pl.when(has_above)
    def _():
        halo(1).start()

    facing = (plane == 0) & faces_beside
    same_far(facing)
    same_beside(outer & faces_beside)
    same_across(inner | facing)

    column = lax.broadcasted_iota(jnp.int32, (GRID_W, 1), 0)
    c_up = join.shape[0] // 9

    def put_row(row, phase, values):
        where = pl.ds((row + 1) * GRID_W, GRID_W)
        planes[phase + 1, where, :] = values.astype(jnp.bfloat16)
        if phase == 3:
            moved = jnp.where(column == 0, 0.0, pltpu.roll(values, 1, axis=0))
            planes[0, where, :] = moved.astype(jnp.bfloat16)
        if phase == 0:
            moved = jnp.where(column == GRID_W - 1, 0.0, pltpu.roll(values, GRID_W - 1, axis=0))
            planes[5, where, :] = moved.astype(jnp.bfloat16)

    for load in loads[10:]:
        load.wait()
    for a in range(4):
        for b in range(4):
            tap = a * 4 + b
            value = dot(tile_four, up4[:, tap * c_up : (tap + 1) * c_up]) + up4_b[...]
            for i in range(rows):
                put_row(4 * i + a, b, value[i * GRID_W : (i + 1) * GRID_W])

    half = joined_ref.shape[2] // 2

    def join_rows(jobs, count):
        windows = [
            jnp.concatenate(
                [
                    planes[phase + col, pl.ds((first + row) * GRID_W, count * GRID_W), :]
                    for row in range(3)
                    for col in range(3)
                ],
                axis=1,
            )
            for phase, first in jobs
        ]
        total = dot(jnp.concatenate(windows, axis=0), join[...])
        for job, (phase, first) in enumerate(jobs):
            for r in range(count):
                at = (job * count + r) * GRID_W
                for h in range(2):
                    joined_f32[first + r, h, pl.ds(phase, GRID_W, stride=4), :] = total[
                        at : at + GRID_W, h * half : (h + 1) * half
                    ]

    def finish_rows(first, count):
        for r in range(first, first + count):
            for h in range(2):
                joined_ref[r, :, h * half : (h + 1) * half] = joined_f32[r, h].astype(jnp.bfloat16)

    out_rows = 4 * rows
    for phase in range(4):
        join_rows([(phase, 1)], out_rows - 2)
    finish_rows(1, out_rows - 2)

    bulk_wait(recv_two, shards - 1, recv_sem.at[2])
    tile_two = in_cells(recv_two)
    c_two = two_ref.shape[2]
    for a in range(2):
        for b in range(2):
            tap = a * 2 + b
            value = dot(tile_two, up2[:, tap * c_two : (tap + 1) * c_two]) + up2_b[...]
            for i in range(rows):
                for h in range(c_two // 128):
                    two_f32[2 * i + a, h, pl.ds(b, GRID_W, stride=2), :] = value[
                        i * GRID_W : (i + 1) * GRID_W, h * 128 : (h + 1) * 128
                    ]
    for r in range(2 * rows):
        for h in range(c_two // 128):
            two_ref[r, :, h * 128 : (h + 1) * 128] = two_f32[r, h].astype(jnp.bfloat16)

    @pl.when(has_below)
    def _():
        halo(0).wait_send()
        halo(1).wait_recv()

    @pl.when(has_above)
    def _():
        halo(1).wait_send()
        halo(0).wait_recv()

    for side, present, a, row in ((0, has_above, 3, -1), (1, has_below, 0, out_rows)):
        for b in range(4):
            tap = a * 4 + b
            value = dot(edge_in[side], up4[:, tap * c_up : (tap + 1) * c_up]) + up4_b[...]
            put_row(row, b, jnp.where(present, value, 0.0))
    join_rows([(phase, first) for first in (0, out_rows - 1) for phase in range(4)], 1)
    finish_rows(0, 1)
    finish_rows(out_rows - 1, 1)

    bulk_wait(recv_same, shards - 1, recv_sem.at[3])
    if not direct:
        same_rows_ref[...] = collect(recv_same)

    for send in (send_four, send_two, send_same):
        bulk_wait(send, shards - 1, send_sem)


def write_kernel(joined_ref, two_ref, same_rows_ref, place_ref, joined_out, two_out, same_out, same, sem):
    copies = [
        pltpu.make_async_copy(src.at[pl.ds(i, 1)], dst.at[pl.ds(i, 1)], sem)
        for src, dst in ((joined_ref, joined_out), (two_ref, two_out))
        for i in range(src.shape[0])
    ]
    for copy in copies:
        copy.start()
    arrived = same_rows_ref[...]
    width = arrived.shape[-1]
    tile = dot(place_ref[...], arrived.reshape(-1, width)).astype(jnp.bfloat16)
    tok = same.shape[0] * GRID_W
    for part in range(same.shape[2] // width):
        for i in range(same.shape[0]):
            at = part * tok + i * GRID_W
            same[i, :, part * width : (part + 1) * width] = tile[at : at + GRID_W]
    copies.append(pltpu.make_async_copy(same, same_out, sem))
    copies[-1].start()
    for copy in copies:
        copy.wait()


def body(
    hidden_states,
    cell_of,
    proj_four_weight,
    proj_four_bias,
    proj_two_weight,
    proj_two_bias,
    proj_same_weight,
    proj_same_bias,
    up4_weight,
    up4_bias,
    up2_weight,
    up2_bias,
    join_weight,
):
    tok = hidden_states.shape[1]
    shards = lax.axis_size("rows")
    per = tok // shards
    rows = tok // GRID_W
    operands = (
        hidden_states,
        cell_of.reshape(shards, tok),
        proj_four_weight,
        proj_four_bias[None, :],
        proj_two_weight,
        proj_two_bias[None, :],
        proj_same_weight,
        proj_same_bias[None, :],
        up4_weight,
        up4_bias[None, :],
        up2_weight,
        up2_bias[None, :],
        join_weight.reshape(-1, join_weight.shape[3]),
    )
    c_four = proj_four_weight.shape[1]
    c_two = proj_two_weight.shape[1]
    c_same = proj_same_weight.shape[1]
    feat = join_weight.shape[3]
    widths = (c_four, c_two, c_same)
    direct = 16 % per == 0 and all(c * per % (16 * 128) == 0 for c in widths)
    block = 16 if direct else per
    split = block // per
    wire = [pltpu.VMEM((shards, block, c // split), jnp.bfloat16) for c in widths]
    spare = pltpu.VMEM((8, 128), jnp.bfloat16) if direct else wire[2]
    arrived = wire[2].shape if direct else (tok, c_same)
    scratch = [pltpu.VMEM(x.shape, x.dtype) for x in operands]
    scratch += [pltpu.VMEM((tok, max(widths)), jnp.float32)]
    scratch += wire + wire[:2] + [spare]
    scratch += [
        pltpu.VMEM((2, GRID_W, c_four), jnp.bfloat16),
        pltpu.VMEM((2, GRID_W, c_four), jnp.bfloat16),
        pltpu.VMEM((6, (4 * rows + 2) * GRID_W, c_four), jnp.bfloat16),
        pltpu.VMEM((4 * rows, 2, 4 * GRID_W, feat // 2), jnp.float32),
        pltpu.VMEM((2 * rows, c_two // 128, 2 * GRID_W, 128), jnp.float32),
        pltpu.SemaphoreType.DMA((5,)),
        pltpu.SemaphoreType.DMA,
        pltpu.SemaphoreType.DMA((4,)),
        pltpu.SemaphoreType.DMA,
        pltpu.SemaphoreType.DMA((2,)),
        pltpu.SemaphoreType.REGULAR,
    ]
    operands = tuple(pltpu.with_memory_space_constraint(x, pltpu.HBM) for x in operands)
    results = pl.pallas_call(
        functools.partial(kernel, shards),
        out_shape=(
            pltpu.VMEM((4 * rows, 4 * GRID_W, feat), jnp.bfloat16),
            pltpu.VMEM((2 * rows, 2 * GRID_W, c_two), jnp.bfloat16),
            pltpu.VMEM(arrived, jnp.bfloat16),
            pltpu.VMEM((split * tok, shards * block), jnp.bfloat16),
        ),
        in_specs=[pl.BlockSpec(memory_space=pl.ANY)] * len(operands),
        out_specs=(pl.BlockSpec(memory_space=pltpu.VMEM),) * 4,
        scratch_shapes=scratch,
        compiler_params=pltpu.CompilerParams(
            collective_id=0, has_side_effects=True, vmem_limit_bytes=40 * 1024 * 1024
        ),
    )(*operands)
    results = tuple(pltpu.with_memory_space_constraint(x, pltpu.VMEM) for x in results)
    return pl.pallas_call(
        write_kernel,
        out_shape=(
            jax.ShapeDtypeStruct((4 * rows, 4 * GRID_W, feat), jnp.bfloat16),
            jax.ShapeDtypeStruct((2 * rows, 2 * GRID_W, c_two), jnp.bfloat16),
            jax.ShapeDtypeStruct((rows, GRID_W, c_same), jnp.bfloat16),
        ),
        in_specs=[pl.BlockSpec(memory_space=pltpu.VMEM)] * 4,
        out_specs=(pl.BlockSpec(memory_space=pl.ANY),) * 3,
        scratch_shapes=[
            pltpu.VMEM((rows, GRID_W, c_same), jnp.bfloat16),
            pltpu.SemaphoreType.DMA,
        ],
        compiler_params=pltpu.CompilerParams(vmem_limit_bytes=8 * 1024 * 1024),
    )(*results)


def solution(mesh):
    rows = P(("img", "rows"), None, None)
    return jax.shard_map(
        body,
        mesh=mesh,
        in_specs=(P(None, ("img", "rows"), None),) + (P(),) * 12,
        out_specs=(rows, rows, rows),
        check_vma=False,
    )
```

```python
import functools

import jax
import jax.numpy as jnp
from jax import lax
from jax.experimental import pallas as pl
from jax.experimental.pallas import tpu as pltpu
from jax.sharding import PartitionSpec as P

GRID_W = 64
MESH = pl.DeviceIdType.MESH


def partner(me, step):
    other = me
    bit = 1
    while bit <= step:
        if step & bit:
            other = other + bit * (1 - 2 * lax.rem(lax.div(me, bit), 2))
        bit *= 2
    return other


def dot(left, right):
    return jnp.dot(left, right, preferred_element_type=jnp.float32)


def kernel(
    shards,
    hid_hbm,
    table_hbm,
    w_four_hbm,
    b_four_hbm,
    w_two_hbm,
    b_two_hbm,
    w_same_hbm,
    b_same_hbm,
    up4_hbm,
    up4_b_hbm,
    up2_hbm,
    up2_b_hbm,
    join_hbm,
    joined_ref,
    two_ref,
    same_rows_ref,
    place_ref,
    hid,
    table,
    w_four,
    b_four,
    w_two,
    b_two,
    w_same,
    b_same,
    up4,
    up4_b,
    up2,
    up2_b,
    join,
    stage,
    send_four,
    send_two,
    send_same,
    recv_four,
    recv_two,
    recv_spare,
    edge_out,
    edge_in,
    planes,
    edge_sum,
    joined_f32,
    two_f32,
    load_sem,
    send_sem,
    recv_sem,
    halo_send_sem,
    halo_recv_sem,
    relay_sem,
):
    me = lax.axis_index("rows")
    img = lax.axis_index("img")
    tok = hid.shape[1]
    per = tok // shards
    rows = tok // GRID_W
    block = send_four.shape[1]
    split = block // per
    direct = block == 16
    recv_same = same_rows_ref if direct else recv_spare
    group = shards // 4
    plane = lax.div(me, group)
    lower = plane < 2
    last = plane == 3
    beside = plane + 1 - 2 * lax.rem(plane, 2)

    names = (
        (table_hbm, table),
        (hid_hbm.at[0], hid.at[0]),
        (w_four_hbm, w_four),
        (b_four_hbm, b_four),
        (hid_hbm.at[1], hid.at[1]),
        (w_two_hbm, w_two),
        (b_two_hbm, b_two),
        (hid_hbm.at[2], hid.at[2]),
        (w_same_hbm, w_same),
        (b_same_hbm, b_same),
        (up4_hbm, up4),
        (up4_b_hbm, up4_b),
        (join_hbm, join),
        (up2_hbm, up2),
        (up2_b_hbm, up2_b),
    )
    stages = (0, 1, 1, 1, 2, 2, 2, 3, 3, 3, 4, 4, 4, 4, 4)
    loads = [pltpu.make_async_copy(src, dst, load_sem.at[stage_of]) for (src, dst), stage_of in zip(names, stages)]

    for load in loads[:4]:
        load.start()

    def row_in(other_plane, i):
        return partner(me, i) + (other_plane - plane) * group

    barrier = pltpu.get_barrier_semaphore()

    def greet(other_plane, some):
        for i in some:
            pl.semaphore_signal(barrier, inc=1, device_id=(img, row_in(other_plane, i)), device_id_type=MESH)

    @pl.when(~last)
    def _():
        greet(jnp.where(lower, 2, 0), range(group))
        greet(jnp.where(lower, 3, 1), range(group))
        greet(beside, range(group))

    greet(plane, range(1, group))

    for load in loads[4:10]:
        load.start()

    loads[0].wait()
    mine = jnp.broadcast_to(table[pl.ds(me, 1), :].astype(jnp.float32), (tok, tok))
    smaller = (mine.T < mine).astype(jnp.float32)
    slot_row = jnp.sum(smaller, axis=0, keepdims=True)
    down = lax.broadcasted_iota(jnp.int32, (tok, tok), 0)
    across = lax.broadcasted_iota(jnp.int32, (tok, tok), 1)
    shard_row = lax.div(table[pl.ds(me, 1), :], tok).astype(jnp.float32)
    packed_row = slot_row + shard_row * (block - per)
    packed_row = jnp.concatenate([packed_row + part * per for part in range(split)], axis=1)
    packed = lax.broadcasted_iota(jnp.int32, (shards * block, split * tok), 0).astype(jnp.float32)
    scatter = (packed == packed_row).astype(jnp.float32).astype(jnp.bfloat16)

    def project(hook, first, weight, bias, send):
        channels = weight.shape[1]
        for load in loads[first : first + 3]:
            load.wait()
        projected = (dot(hid[hook], weight[...]) + bias[...]).astype(jnp.bfloat16)
        width = channels // split
        stacked = [projected[:, part * width : (part + 1) * width] for part in range(split)]
        ordered = dot(scatter, jnp.concatenate(stacked, axis=0))
        if first == 1:
            for load in loads[10:]:
                load.start()
        if direct:
            send[...] = ordered.astype(jnp.bfloat16).reshape(send.shape)
        else:
            stage[:, :channels] = ordered
            for shard in range(shards):
                send[shard] = stage[shard * per : (shard + 1) * per, :channels].astype(jnp.bfloat16)

    def push(index, send, recv, other):
        pltpu.make_async_remote_copy(
            src_ref=send.at[other],
            dst_ref=recv.at[me],
            send_sem=send_sem,
            recv_sem=recv_sem.at[jnp.where(lower, 0, 1) if index == 0 else index + 1],
            device_id=(img, other),
            device_id_type=MESH,
        ).start()

    def exchange(index, send, recv, other_plane, some):
        for i in reversed(some):
            push(index, send, recv, row_in(other_plane, i))

    def exchange_early(index, send, recv):
        exchange(index, send, recv, jnp.where(lower, 2, 0), range(group))

        @pl.when(~lower)
        def _():
            exchange(index, send, recv, 1, range(group))

        @pl.when(plane != 2)
        def _():
            exchange(index, send, recv, beside, range(group))

        exchange(index, send, recv, plane, range(1, group))
        recv[me] = send[me]

    def bulk_wait(buffer, count, sem):
        part = buffer.at[pl.ds(0, count)]
        pltpu.make_async_copy(part, part, sem).wait()

    def arrive(recv, planes_in, own, sem):
        for mine in (0, 1):

            @pl.when(own == (mine == 1))
            def _():
                bulk_wait(recv, planes_in * group - mine, recv_sem.at[sem])

    def collect(recv):
        width = recv.shape[2]
        if direct:
            return recv[...].reshape(shards * block, width)
        for shard in range(shards):
            stage[shard * per : (shard + 1) * per, :width] = recv[shard].astype(jnp.float32)
        return stage[:, :width].astype(jnp.bfloat16)

    def in_cells(recv):
        tile = dot(place, collect(recv)).astype(jnp.bfloat16)
        return jnp.concatenate([tile[part * tok : (part + 1) * tok] for part in range(split)], axis=1)

    project(0, 1, w_four, b_four, send_four)

    @pl.when(plane >= 2)
    def _():
        pl.semaphore_wait(barrier, jnp.where(last, shards - 1, shards - 1 - group))

        @pl.when(last)
        def _():
            for other_plane in (0, 1, 2):
                to = row_in(other_plane, 0)
                pl.semaphore_signal(relay_sem, inc=1, device_id=(img, to), device_id_type=MESH)

        exchange_early(0, send_four, recv_four)

    project(1, 4, w_two, b_two, send_two)

    @pl.when(plane == 1)
    def _():
        pl.semaphore_wait(barrier, shards - 1 - group)
        exchange_early(0, send_four, recv_four)

    @pl.when(plane > 0)
    def _():
        exchange_early(1, send_two, recv_two)

    project(2, 7, w_same, b_same, send_same)

    @pl.when(plane == 0)
    def _():
        pl.semaphore_wait(barrier, shards - 1 - group)
        exchange_early(0, send_four, recv_four)
        exchange_early(1, send_two, recv_two)

    other_rows = range(group // 2)
    first_rows = range(group // 2, group)

    @pl.when(plane == 1)
    def _():
        exchange(2, send_same, recv_same, 2, first_rows)

    @pl.when(~last)
    def _():
        pl.semaphore_wait(relay_sem, 1)
        exchange(0, send_four, recv_four, 3, range(group))
        exchange(1, send_two, recv_two, 3, range(group))

    spot = lax.rem(me, group)
    faces_beside = jnp.where(lax.rem(plane, 2) == 0, spot == group - 1, spot == 0)

    inner = (plane == 1) | (plane == 2)
    outer = ~inner
    faces_across = ((plane == 1) & (spot == group - 1)) | ((plane == 2) & (spot == 0))

    def same_far(some, rows_to=range(group)):
        @pl.when(some)
        def _():
            exchange(2, send_same, recv_same, jnp.where(lower, 3, 0), rows_to)

    def same_beside(some):
        @pl.when(some)
        def _():
            exchange(2, send_same, recv_same, beside, range(group))

    def same_across(some):
        @pl.when(some & (plane != 1))
        def _():
            exchange(2, send_same, recv_same, jnp.where(lower, 2, 1), first_rows)

        @pl.when(some)
        def _():
            exchange(2, send_same, recv_same, jnp.where(lower, 2, 1), other_rows)

    same_far(inner)
    same_beside(inner)
    same_across(inner & ~faces_across)
    exchange(2, send_same, recv_same, plane, range(1, group))
    recv_same[me] = send_same[me]

    wanted = down + me * tok
    source = jnp.zeros((tok, tok), jnp.float32)
    for shard in range(1, shards):
        source = source + jnp.where(table[shard : shard + 1, :] == wanted, float(shard), 0.0)
    source = jnp.broadcast_to(jnp.sum(source, axis=1, keepdims=True), (tok, tok))
    earlier = jnp.where((source == source.T) & (across < down), 1.0, 0.0)
    slot_col = source[:, :1] * block + jnp.sum(earlier, axis=1, keepdims=True)
    slot_col = jnp.concatenate([slot_col + part * per for part in range(split)], axis=0)
    packed = lax.broadcasted_iota(jnp.int32, (split * tok, shards * block), 1).astype(jnp.float32)
    place = (packed == slot_col).astype(jnp.float32).astype(jnp.bfloat16)
    place_ref[...] = place

    arrive(recv_four, 2, ~lower, 1)
    same_far(last)
    same_beside(last & ~faces_beside)
    same_across(last)
    arrive(recv_four, 2, lower, 0)
    free = (plane == 0) & ~faces_beside
    same_far(free)
    same_beside(free)
    same_across(free)
    tile_four = in_cells(recv_four)
    edge_out[0] = tile_four[:GRID_W]
    edge_out[1] = tile_four[tok - GRID_W :]

    def halo(side):
        return pltpu.make_async_remote_copy(
            src_ref=edge_out.at[1 - side],
            dst_ref=edge_in.at[side],
            send_sem=halo_send_sem,
            recv_sem=halo_recv_sem.at[side],
            device_id=(img, me + 1 if side == 0 else me - 1),
            device_id_type=MESH,
        )

    has_below = me < shards - 1
    has_above = me > 0

    @pl.when(has_below)
    def _():
        halo(0).start()

    @pl.when(has_above)
    def _():
        halo(1).start()

    facing = (plane == 0) & faces_beside
    same_far(facing)
    same_beside(outer & faces_beside)
    same_across(faces_across | facing)

    column = lax.broadcasted_iota(jnp.int32, (GRID_W, 1), 0)
    c_up = join.shape[0] // 9

    def put_row(row, phase, values):
        where = pl.ds((row + 1) * GRID_W, GRID_W)
        planes[phase + 1, where, :] = values.astype(jnp.bfloat16)
        if phase == 3:
            moved = jnp.where(column == 0, 0.0, pltpu.roll(values, 1, axis=0))
            planes[0, where, :] = moved.astype(jnp.bfloat16)
        if phase == 0:
            moved = jnp.where(column == GRID_W - 1, 0.0, pltpu.roll(values, GRID_W - 1, axis=0))
            planes[5, where, :] = moved.astype(jnp.bfloat16)

    for load in loads[10:]:
        load.wait()
    for a in range(4):
        for b in range(4):
            tap = a * 4 + b
            value = dot(tile_four, up4[:, tap * c_up : (tap + 1) * c_up]) + up4_b[...]
            for i in range(rows):
                put_row(4 * i + a, b, value[i * GRID_W : (i + 1) * GRID_W])

    half = joined_ref.shape[2] // 2

    def join_rows(jobs, count):
        windows = [
            jnp.concatenate(
                [
                    planes[phase + col, pl.ds((first + row) * GRID_W, count * GRID_W), :]
                    for row in range(3)
                    for col in range(3)
                ],
                axis=1,
            )
            for phase, first in jobs
        ]
        total = dot(jnp.concatenate(windows, axis=0), join[...])
        for job, (phase, first) in enumerate(jobs):
            for r in range(count):
                at = (job * count + r) * GRID_W
                for h in range(2):
                    joined_f32[first + r, h, pl.ds(phase, GRID_W, stride=4), :] = total[
                        at : at + GRID_W, h * half : (h + 1) * half
                    ]

    def finish_rows(first, count):
        for r in range(first, first + count):
            for h in range(2):
                joined_ref[r, :, h * half : (h + 1) * half] = joined_f32[r, h].astype(jnp.bfloat16)

    out_rows = 4 * rows
    for phase in range(4):
        join_rows([(phase, 1)], out_rows - 2)
    finish_rows(1, out_rows - 2)

    bulk_wait(recv_two, shards - 1, recv_sem.at[2])
    tile_two = in_cells(recv_two)
    c_two = two_ref.shape[2]
    for a in range(2):
        for b in range(2):
            tap = a * 2 + b
            value = dot(tile_two, up2[:, tap * c_two : (tap + 1) * c_two]) + up2_b[...]
            for i in range(rows):
                for h in range(c_two // 128):
                    two_f32[2 * i + a, h, pl.ds(b, GRID_W, stride=2), :] = value[
                        i * GRID_W : (i + 1) * GRID_W, h * 128 : (h + 1) * 128
                    ]
    for r in range(2 * rows):
        for h in range(c_two // 128):
            two_ref[r, :, h * 128 : (h + 1) * 128] = two_f32[r, h].astype(jnp.bfloat16)

    def edge_product(first, tap_rows):
        windows = [
            jnp.concatenate(
                [
                    planes[phase + col, pl.ds((first + row) * GRID_W, GRID_W), :]
                    for row in tap_rows
                    for col in range(3)
                ],
                axis=1,
            )
            for phase in range(4)
        ]
        weights = join[tap_rows[0] * 3 * c_up : (tap_rows[-1] + 1) * 3 * c_up, :]
        return dot(jnp.concatenate(windows, axis=0), weights)

    borders = ((0, (1, 2), (0,)), (out_rows - 1, (0, 1), (2,)))
    for side, (first, inside, beyond) in enumerate(borders):
        edge_sum[side] = edge_product(first, inside)

    @pl.when(has_below)
    def _():
        halo(0).wait_send()
        halo(1).wait_recv()

    @pl.when(has_above)
    def _():
        halo(1).wait_send()
        halo(0).wait_recv()

    for side, present, a, row in ((0, has_above, 3, -1), (1, has_below, 0, out_rows)):
        for b in range(4):
            tap = a * 4 + b
            value = dot(edge_in[side], up4[:, tap * c_up : (tap + 1) * c_up]) + up4_b[...]
            put_row(row, b, jnp.where(present, value, 0.0))
    for side, (first, inside, beyond) in enumerate(borders):
        total = edge_sum[side] + edge_product(first, beyond)
        for phase in range(4):
            for h in range(2):
                joined_f32[first, h, pl.ds(phase, GRID_W, stride=4), :] = total[
                    phase * GRID_W : (phase + 1) * GRID_W, h * half : (h + 1) * half
                ]
    finish_rows(0, 1)
    finish_rows(out_rows - 1, 1)

    bulk_wait(recv_same, shards - 1, recv_sem.at[3])
    if not direct:
        same_rows_ref[...] = collect(recv_same)

    for send in (send_four, send_two, send_same):
        bulk_wait(send, shards - 1, send_sem)


def write_kernel(joined_ref, two_ref, same_rows_ref, place_ref, joined_out, two_out, same_out, same, sem):
    copies = [
        pltpu.make_async_copy(src.at[pl.ds(i, 1)], dst.at[pl.ds(i, 1)], sem)
        for src, dst in ((joined_ref, joined_out), (two_ref, two_out))
        for i in range(src.shape[0])
    ]
    for copy in copies:
        copy.start()
    arrived = same_rows_ref[...]
    width = arrived.shape[-1]
    tile = dot(place_ref[...], arrived.reshape(-1, width)).astype(jnp.bfloat16)
    tok = same.shape[0] * GRID_W
    for part in range(same.shape[2] // width):
        for i in range(same.shape[0]):
            at = part * tok + i * GRID_W
            same[i, :, part * width : (part + 1) * width] = tile[at : at + GRID_W]
    copies.append(pltpu.make_async_copy(same, same_out, sem))
    copies[-1].start()
    for copy in copies:
        copy.wait()


def body(
    hidden_states,
    cell_of,
    proj_four_weight,
    proj_four_bias,
    proj_two_weight,
    proj_two_bias,
    proj_same_weight,
    proj_same_bias,
    up4_weight,
    up4_bias,
    up2_weight,
    up2_bias,
    join_weight,
):
    tok = hidden_states.shape[1]
    shards = lax.axis_size("rows")
    per = tok // shards
    rows = tok // GRID_W
    operands = (
        hidden_states,
        cell_of.reshape(shards, tok),
        proj_four_weight,
        proj_four_bias[None, :],
        proj_two_weight,
        proj_two_bias[None, :],
        proj_same_weight,
        proj_same_bias[None, :],
        up4_weight,
        up4_bias[None, :],
        up2_weight,
        up2_bias[None, :],
        join_weight.reshape(-1, join_weight.shape[3]),
    )
    c_four = proj_four_weight.shape[1]
    c_two = proj_two_weight.shape[1]
    c_same = proj_same_weight.shape[1]
    feat = join_weight.shape[3]
    widths = (c_four, c_two, c_same)
    direct = 16 % per == 0 and all(c * per % (16 * 128) == 0 for c in widths)
    block = 16 if direct else per
    split = block // per
    wire = [pltpu.VMEM((shards, block, c // split), jnp.bfloat16) for c in widths]
    spare = pltpu.VMEM((8, 128), jnp.bfloat16) if direct else wire[2]
    arrived = wire[2].shape if direct else (tok, c_same)
    scratch = [pltpu.VMEM(x.shape, x.dtype) for x in operands]
    scratch += [pltpu.VMEM((tok, max(widths)), jnp.float32)]
    scratch += wire + wire[:2] + [spare]
    scratch += [
        pltpu.VMEM((2, GRID_W, c_four), jnp.bfloat16),
        pltpu.VMEM((2, GRID_W, c_four), jnp.bfloat16),
        pltpu.VMEM((6, (4 * rows + 2) * GRID_W, c_four), jnp.bfloat16),
        pltpu.VMEM((2, 4 * GRID_W, feat), jnp.float32),
        pltpu.VMEM((4 * rows, 2, 4 * GRID_W, feat // 2), jnp.float32),
        pltpu.VMEM((2 * rows, c_two // 128, 2 * GRID_W, 128), jnp.float32),
        pltpu.SemaphoreType.DMA((5,)),
        pltpu.SemaphoreType.DMA,
        pltpu.SemaphoreType.DMA((4,)),
        pltpu.SemaphoreType.DMA,
        pltpu.SemaphoreType.DMA((2,)),
        pltpu.SemaphoreType.REGULAR,
    ]
    operands = tuple(pltpu.with_memory_space_constraint(x, pltpu.HBM) for x in operands)
    results = pl.pallas_call(
        functools.partial(kernel, shards),
        out_shape=(
            pltpu.VMEM((4 * rows, 4 * GRID_W, feat), jnp.bfloat16),
            pltpu.VMEM((2 * rows, 2 * GRID_W, c_two), jnp.bfloat16),
            pltpu.VMEM(arrived, jnp.bfloat16),
            pltpu.VMEM((split * tok, shards * block), jnp.bfloat16),
        ),
        in_specs=[pl.BlockSpec(memory_space=pl.ANY)] * len(operands),
        out_specs=(pl.BlockSpec(memory_space=pltpu.VMEM),) * 4,
        scratch_shapes=scratch,
        compiler_params=pltpu.CompilerParams(
            collective_id=0, has_side_effects=True, vmem_limit_bytes=40 * 1024 * 1024
        ),
    )(*operands)
    results = tuple(pltpu.with_memory_space_constraint(x, pltpu.VMEM) for x in results)
    return pl.pallas_call(
        write_kernel,
        out_shape=(
            jax.ShapeDtypeStruct((4 * rows, 4 * GRID_W, feat), jnp.bfloat16),
            jax.ShapeDtypeStruct((2 * rows, 2 * GRID_W, c_two), jnp.bfloat16),
            jax.ShapeDtypeStruct((rows, GRID_W, c_same), jnp.bfloat16),
        ),
        in_specs=[pl.BlockSpec(memory_space=pltpu.VMEM)] * 4,
        out_specs=(pl.BlockSpec(memory_space=pl.ANY),) * 3,
        scratch_shapes=[
            pltpu.VMEM((rows, GRID_W, c_same), jnp.bfloat16),
            pltpu.SemaphoreType.DMA,
        ],
        compiler_params=pltpu.CompilerParams(vmem_limit_bytes=8 * 1024 * 1024),
    )(*results)


def solution(mesh):
    rows = P(("img", "rows"), None, None)
    return jax.shard_map(
        body,
        mesh=mesh,
        in_specs=(P(None, ("img", "rows"), None),) + (P(),) * 12,
        out_specs=(rows, rows, rows),
        check_vma=False,
    )
```

```python
import functools

import jax
import jax.numpy as jnp
from jax import lax
from jax.experimental import pallas as pl
from jax.experimental.pallas import tpu as pltpu
from jax.sharding import PartitionSpec as P

GRID_W = 64
MESH = pl.DeviceIdType.MESH


def partner(me, step):
    other = me
    bit = 1
    while bit <= step:
        if step & bit:
            other = other + bit * (1 - 2 * lax.rem(lax.div(me, bit), 2))
        bit *= 2
    return other


def dot(left, right):
    return jnp.dot(left, right, preferred_element_type=jnp.float32)


def kernel(
    shards,
    hid_hbm,
    table_hbm,
    w_four_hbm,
    b_four_hbm,
    w_two_hbm,
    b_two_hbm,
    w_same_hbm,
    b_same_hbm,
    up4_hbm,
    up4_b_hbm,
    up2_hbm,
    up2_b_hbm,
    join_hbm,
    joined_ref,
    two_ref,
    same_rows_ref,
    place_ref,
    hid,
    table,
    w_four,
    b_four,
    w_two,
    b_two,
    w_same,
    b_same,
    up4,
    up4_b,
    up2,
    up2_b,
    join,
    stage,
    send_four,
    send_two,
    send_same,
    recv_four,
    recv_two,
    recv_spare,
    edge_out,
    edge_in,
    planes,
    edge_sum,
    joined_f32,
    two_f32,
    load_sem,
    send_sem,
    recv_sem,
    halo_send_sem,
    halo_recv_sem,
    relay_sem,
):
    me = lax.axis_index("rows")
    img = lax.axis_index("img")
    tok = hid.shape[1]
    per = tok // shards
    rows = tok // GRID_W
    block = send_four.shape[1]
    split = block // per
    direct = block == 16
    recv_same = same_rows_ref if direct else recv_spare
    group = shards // 4
    plane = lax.div(me, group)
    lower = plane < 2
    last = plane == 3
    beside = plane + 1 - 2 * lax.rem(plane, 2)

    names = (
        (table_hbm, table),
        (hid_hbm.at[0], hid.at[0]),
        (w_four_hbm, w_four),
        (b_four_hbm, b_four),
        (hid_hbm.at[1], hid.at[1]),
        (w_two_hbm, w_two),
        (b_two_hbm, b_two),
        (hid_hbm.at[2], hid.at[2]),
        (w_same_hbm, w_same),
        (b_same_hbm, b_same),
        (up4_hbm, up4),
        (up4_b_hbm, up4_b),
        (join_hbm, join),
        (up2_hbm, up2),
        (up2_b_hbm, up2_b),
    )
    stages = (0, 1, 1, 1, 2, 2, 2, 3, 3, 3, 4, 4, 4, 4, 4)
    loads = [pltpu.make_async_copy(src, dst, load_sem.at[stage_of]) for (src, dst), stage_of in zip(names, stages)]

    for load in loads[:4]:
        load.start()

    def row_in(other_plane, i):
        return partner(me, i) + (other_plane - plane) * group

    barrier = pltpu.get_barrier_semaphore()

    def greet(other_plane, some):
        for i in some:
            pl.semaphore_signal(barrier, inc=1, device_id=(img, row_in(other_plane, i)), device_id_type=MESH)

    @pl.when(~last)
    def _():
        greet(jnp.where(lower, 2, 0), range(group))
        greet(jnp.where(lower, 3, 1), range(group))
        greet(beside, range(group))

    greet(plane, range(1, group))

    for load in loads[4:10]:
        load.start()

    loads[0].wait()
    mine = jnp.broadcast_to(table[pl.ds(me, 1), :].astype(jnp.float32), (tok, tok))
    smaller = (mine.T < mine).astype(jnp.float32)
    slot_row = jnp.sum(smaller, axis=0, keepdims=True)
    down = lax.broadcasted_iota(jnp.int32, (tok, tok), 0)
    across = lax.broadcasted_iota(jnp.int32, (tok, tok), 1)
    shard_row = lax.div(table[pl.ds(me, 1), :], tok).astype(jnp.float32)
    packed_row = slot_row + shard_row * (block - per)
    packed_row = jnp.concatenate([packed_row + part * per for part in range(split)], axis=1)
    packed = lax.broadcasted_iota(jnp.int32, (shards * block, split * tok), 0).astype(jnp.float32)
    scatter = (packed == packed_row).astype(jnp.float32).astype(jnp.bfloat16)

    def project(hook, first, weight, bias, send):
        channels = weight.shape[1]
        for load in loads[first : first + 3]:
            load.wait()
        projected = (dot(hid[hook], weight[...]) + bias[...]).astype(jnp.bfloat16)
        width = channels // split
        stacked = [projected[:, part * width : (part + 1) * width] for part in range(split)]
        ordered = dot(scatter, jnp.concatenate(stacked, axis=0))
        if first == 1:
            for load in loads[10:]:
                load.start()
        if direct:
            send[...] = ordered.astype(jnp.bfloat16).reshape(send.shape)
        else:
            stage[:, :channels] = ordered
            for shard in range(shards):
                send[shard] = stage[shard * per : (shard + 1) * per, :channels].astype(jnp.bfloat16)

    def push(index, send, recv, other):
        pltpu.make_async_remote_copy(
            src_ref=send.at[other],
            dst_ref=recv.at[me],
            send_sem=send_sem,
            recv_sem=recv_sem.at[jnp.where(lower, 0, 1) if index == 0 else index + 1],
            device_id=(img, other),
            device_id_type=MESH,
        ).start()

    def exchange(index, send, recv, other_plane, some):
        for i in reversed(some):
            push(index, send, recv, row_in(other_plane, i))

    def exchange_early(index, send, recv):
        exchange(index, send, recv, jnp.where(lower, 2, 0), range(group))

        @pl.when(~lower)
        def _():
            exchange(index, send, recv, 1, range(group))

        @pl.when(plane != 2)
        def _():
            exchange(index, send, recv, beside, range(group))

        exchange(index, send, recv, plane, range(1, group))
        recv[me] = send[me]

    def bulk_wait(buffer, count, sem):
        part = buffer.at[pl.ds(0, count)]
        pltpu.make_async_copy(part, part, sem).wait()

    def arrive(recv, planes_in, own, sem):
        for mine in (0, 1):

            @pl.when(own == (mine == 1))
            def _():
                bulk_wait(recv, planes_in * group - mine, recv_sem.at[sem])

    def collect(recv):
        width = recv.shape[2]
        if direct:
            return recv[...].reshape(shards * block, width)
        for shard in range(shards):
            stage[shard * per : (shard + 1) * per, :width] = recv[shard].astype(jnp.float32)
        return stage[:, :width].astype(jnp.bfloat16)

    def in_cells(recv):
        tile = dot(place, collect(recv)).astype(jnp.bfloat16)
        return jnp.concatenate([tile[part * tok : (part + 1) * tok] for part in range(split)], axis=1)

    project(0, 1, w_four, b_four, send_four)

    @pl.when(plane >= 2)
    def _():
        pl.semaphore_wait(barrier, jnp.where(last, shards - 1, shards - 1 - group))

        @pl.when(last)
        def _():
            for other_plane in (0, 1, 2):
                to = row_in(other_plane, 0)
                pl.semaphore_signal(relay_sem, inc=1, device_id=(img, to), device_id_type=MESH)

        exchange_early(0, send_four, recv_four)

    project(1, 4, w_two, b_two, send_two)

    @pl.when(plane == 1)
    def _():
        pl.semaphore_wait(barrier, shards - 1 - group)
        exchange_early(0, send_four, recv_four)

    @pl.when(plane > 0)
    def _():
        exchange_early(1, send_two, recv_two)

    project(2, 7, w_same, b_same, send_same)

    @pl.when(plane == 0)
    def _():
        pl.semaphore_wait(barrier, shards - 1 - group)
        exchange_early(0, send_four, recv_four)
        exchange_early(1, send_two, recv_two)

    other_rows = range(group // 2)
    first_rows = range(group // 2, group)

    @pl.when(plane == 1)
    def _():
        exchange(2, send_same, recv_same, 2, first_rows)

    @pl.when(~last)
    def _():
        pl.semaphore_wait(relay_sem, 1)
        exchange(0, send_four, recv_four, 3, range(group))
        exchange(1, send_two, recv_two, 3, range(group))

    spot = lax.rem(me, group)
    faces_beside = jnp.where(lax.rem(plane, 2) == 0, spot == group - 1, spot == 0)

    inner = (plane == 1) | (plane == 2)
    outer = ~inner
    faces_across = ((plane == 1) & (spot == group - 1)) | ((plane == 2) & (spot == 0))

    def same_far(some, rows_to=range(group)):
        @pl.when(some)
        def _():
            exchange(2, send_same, recv_same, jnp.where(lower, 3, 0), rows_to)

    def same_beside(some):
        @pl.when(some)
        def _():
            exchange(2, send_same, recv_same, beside, range(group))

    def same_across(some):
        @pl.when(some & (plane != 1))
        def _():
            exchange(2, send_same, recv_same, jnp.where(lower, 2, 1), first_rows)

        @pl.when(some)
        def _():
            exchange(2, send_same, recv_same, jnp.where(lower, 2, 1), other_rows)

    same_far(inner)
    same_beside(inner)
    same_across(inner & ~faces_across)
    exchange(2, send_same, recv_same, plane, range(1, group))
    recv_same[me] = send_same[me]

    wanted = down + me * tok
    source = jnp.zeros((tok, tok), jnp.float32)
    for shard in range(1, shards):
        source = source + jnp.where(table[shard : shard + 1, :] == wanted, float(shard), 0.0)
    source = jnp.broadcast_to(jnp.sum(source, axis=1, keepdims=True), (tok, tok))
    earlier = jnp.where((source == source.T) & (across < down), 1.0, 0.0)
    slot_col = source[:, :1] * block + jnp.sum(earlier, axis=1, keepdims=True)
    slot_col = jnp.concatenate([slot_col + part * per for part in range(split)], axis=0)
    packed = lax.broadcasted_iota(jnp.int32, (split * tok, shards * block), 1).astype(jnp.float32)
    place = (packed == slot_col).astype(jnp.float32).astype(jnp.bfloat16)
    place_ref[...] = place

    arrive(recv_four, 2, ~lower, 1)
    same_far(last)
    same_beside(last)
    same_across(last)
    arrive(recv_four, 2, lower, 0)
    free = (plane == 0) & ~faces_beside
    same_far(free)
    same_beside(free)
    same_across(free)
    tile_four = in_cells(recv_four)
    edge_out[0] = tile_four[:GRID_W]
    edge_out[1] = tile_four[tok - GRID_W :]

    def halo(side):
        return pltpu.make_async_remote_copy(
            src_ref=edge_out.at[1 - side],
            dst_ref=edge_in.at[side],
            send_sem=halo_send_sem,
            recv_sem=halo_recv_sem.at[side],
            device_id=(img, me + 1 if side == 0 else me - 1),
            device_id_type=MESH,
        )

    has_below = me < shards - 1
    has_above = me > 0

    @pl.when(has_below)
    def _():
        halo(0).start()

    @pl.when(has_above)
    def _():
        halo(1).start()

    facing = (plane == 0) & faces_beside
    same_far(facing)
    same_beside((plane == 0) & faces_beside)
    same_across(faces_across | facing)

    column = lax.broadcasted_iota(jnp.int32, (GRID_W, 1), 0)
    c_up = join.shape[0] // 9

    def put_row(row, phase, values):
        where = pl.ds((row + 1) * GRID_W, GRID_W)
        planes[phase + 1, where, :] = values.astype(jnp.bfloat16)
        if phase == 3:
            moved = jnp.where(column == 0, 0.0, pltpu.roll(values, 1, axis=0))
            planes[0, where, :] = moved.astype(jnp.bfloat16)
        if phase == 0:
            moved = jnp.where(column == GRID_W - 1, 0.0, pltpu.roll(values, GRID_W - 1, axis=0))
            planes[5, where, :] = moved.astype(jnp.bfloat16)

    for load in loads[10:]:
        load.wait()
    for a in range(4):
        for b in range(4):
            tap = a * 4 + b
            value = dot(tile_four, up4[:, tap * c_up : (tap + 1) * c_up]) + up4_b[...]
            for i in range(rows):
                put_row(4 * i + a, b, value[i * GRID_W : (i + 1) * GRID_W])

    half = joined_ref.shape[2] // 2

    def join_rows(jobs, count):
        windows = [
            jnp.concatenate(
                [
                    planes[phase + col, pl.ds((first + row) * GRID_W, count * GRID_W), :]
                    for row in range(3)
                    for col in range(3)
                ],
                axis=1,
            )
            for phase, first in jobs
        ]
        total = dot(jnp.concatenate(windows, axis=0), join[...])
        for job, (phase, first) in enumerate(jobs):
            for r in range(count):
                at = (job * count + r) * GRID_W
                for h in range(2):
                    joined_f32[first + r, h, pl.ds(phase, GRID_W, stride=4), :] = total[
                        at : at + GRID_W, h * half : (h + 1) * half
                    ]

    def finish_rows(first, count):
        for r in range(first, first + count):
            for h in range(2):
                joined_ref[r, :, h * half : (h + 1) * half] = joined_f32[r, h].astype(jnp.bfloat16)

    out_rows = 4 * rows
    for phase in range(4):
        join_rows([(phase, 1)], out_rows - 2)
    finish_rows(1, out_rows - 2)

    bulk_wait(recv_two, shards - 1, recv_sem.at[2])
    tile_two = in_cells(recv_two)
    c_two = two_ref.shape[2]
    for a in range(2):
        for b in range(2):
            tap = a * 2 + b
            value = dot(tile_two, up2[:, tap * c_two : (tap + 1) * c_two]) + up2_b[...]
            for i in range(rows):
                for h in range(c_two // 128):
                    two_f32[2 * i + a, h, pl.ds(b, GRID_W, stride=2), :] = value[
                        i * GRID_W : (i + 1) * GRID_W, h * 128 : (h + 1) * 128
                    ]
    for r in range(2 * rows):
        for h in range(c_two // 128):
            two_ref[r, :, h * 128 : (h + 1) * 128] = two_f32[r, h].astype(jnp.bfloat16)

    def edge_product(first, tap_rows):
        windows = [
            jnp.concatenate(
                [
                    planes[phase + col, pl.ds((first + row) * GRID_W, GRID_W), :]
                    for row in tap_rows
                    for col in range(3)
                ],
                axis=1,
            )
            for phase in range(4)
        ]
        weights = join[tap_rows[0] * 3 * c_up : (tap_rows[-1] + 1) * 3 * c_up, :]
        return dot(jnp.concatenate(windows, axis=0), weights)

    borders = ((0, (1, 2), (0,)), (out_rows - 1, (0, 1), (2,)))
    for side, (first, inside, beyond) in enumerate(borders):
        edge_sum[side] = edge_product(first, inside)

    @pl.when(has_below)
    def _():
        halo(0).wait_send()
        halo(1).wait_recv()

    @pl.when(has_above)
    def _():
        halo(1).wait_send()
        halo(0).wait_recv()

    for side, present, a, row in ((0, has_above, 3, -1), (1, has_below, 0, out_rows)):
        for b in range(4):
            tap = a * 4 + b
            value = dot(edge_in[side], up4[:, tap * c_up : (tap + 1) * c_up]) + up4_b[...]
            put_row(row, b, jnp.where(present, value, 0.0))
    for side, (first, inside, beyond) in enumerate(borders):
        total = edge_sum[side] + edge_product(first, beyond)
        for phase in range(4):
            for h in range(2):
                joined_f32[first, h, pl.ds(phase, GRID_W, stride=4), :] = total[
                    phase * GRID_W : (phase + 1) * GRID_W, h * half : (h + 1) * half
                ]
    finish_rows(0, 1)
    finish_rows(out_rows - 1, 1)

    bulk_wait(recv_same, shards - 1, recv_sem.at[3])
    if not direct:
        same_rows_ref[...] = collect(recv_same)

    for send in (send_four, send_two, send_same):
        bulk_wait(send, shards - 1, send_sem)


def write_kernel(joined_ref, two_ref, same_rows_ref, place_ref, joined_out, two_out, same_out, same, sem):
    copies = [
        pltpu.make_async_copy(src.at[pl.ds(i, 1)], dst.at[pl.ds(i, 1)], sem)
        for src, dst in ((joined_ref, joined_out), (two_ref, two_out))
        for i in range(src.shape[0])
    ]
    for copy in copies:
        copy.start()
    arrived = same_rows_ref[...]
    width = arrived.shape[-1]
    tile = dot(place_ref[...], arrived.reshape(-1, width)).astype(jnp.bfloat16)
    tok = same.shape[0] * GRID_W
    for part in range(same.shape[2] // width):
        for i in range(same.shape[0]):
            at = part * tok + i * GRID_W
            same[i, :, part * width : (part + 1) * width] = tile[at : at + GRID_W]
    copies.append(pltpu.make_async_copy(same, same_out, sem))
    copies[-1].start()
    for copy in copies:
        copy.wait()


def body(
    hidden_states,
    cell_of,
    proj_four_weight,
    proj_four_bias,
    proj_two_weight,
    proj_two_bias,
    proj_same_weight,
    proj_same_bias,
    up4_weight,
    up4_bias,
    up2_weight,
    up2_bias,
    join_weight,
):
    tok = hidden_states.shape[1]
    shards = lax.axis_size("rows")
    per = tok // shards
    rows = tok // GRID_W
    operands = (
        hidden_states,
        cell_of.reshape(shards, tok),
        proj_four_weight,
        proj_four_bias[None, :],
        proj_two_weight,
        proj_two_bias[None, :],
        proj_same_weight,
        proj_same_bias[None, :],
        up4_weight,
        up4_bias[None, :],
        up2_weight,
        up2_bias[None, :],
        join_weight.reshape(-1, join_weight.shape[3]),
    )
    c_four = proj_four_weight.shape[1]
    c_two = proj_two_weight.shape[1]
    c_same = proj_same_weight.shape[1]
    feat = join_weight.shape[3]
    widths = (c_four, c_two, c_same)
    direct = 16 % per == 0 and all(c * per % (16 * 128) == 0 for c in widths)
    block = 16 if direct else per
    split = block // per
    wire = [pltpu.VMEM((shards, block, c // split), jnp.bfloat16) for c in widths]
    spare = pltpu.VMEM((8, 128), jnp.bfloat16) if direct else wire[2]
    arrived = wire[2].shape if direct else (tok, c_same)
    scratch = [pltpu.VMEM(x.shape, x.dtype) for x in operands]
    scratch += [pltpu.VMEM((tok, max(widths)), jnp.float32)]
    scratch += wire + wire[:2] + [spare]
    scratch += [
        pltpu.VMEM((2, GRID_W, c_four), jnp.bfloat16),
        pltpu.VMEM((2, GRID_W, c_four), jnp.bfloat16),
        pltpu.VMEM((6, (4 * rows + 2) * GRID_W, c_four), jnp.bfloat16),
        pltpu.VMEM((2, 4 * GRID_W, feat), jnp.float32),
        pltpu.VMEM((4 * rows, 2, 4 * GRID_W, feat // 2), jnp.float32),
        pltpu.VMEM((2 * rows, c_two // 128, 2 * GRID_W, 128), jnp.float32),
        pltpu.SemaphoreType.DMA((5,)),
        pltpu.SemaphoreType.DMA,
        pltpu.SemaphoreType.DMA((4,)),
        pltpu.SemaphoreType.DMA,
        pltpu.SemaphoreType.DMA((2,)),
        pltpu.SemaphoreType.REGULAR,
    ]
    operands = tuple(pltpu.with_memory_space_constraint(x, pltpu.HBM) for x in operands)
    results = pl.pallas_call(
        functools.partial(kernel, shards),
        out_shape=(
            pltpu.VMEM((4 * rows, 4 * GRID_W, feat), jnp.bfloat16),
            pltpu.VMEM((2 * rows, 2 * GRID_W, c_two), jnp.bfloat16),
            pltpu.VMEM(arrived, jnp.bfloat16),
            pltpu.VMEM((split * tok, shards * block), jnp.bfloat16),
        ),
        in_specs=[pl.BlockSpec(memory_space=pl.ANY)] * len(operands),
        out_specs=(pl.BlockSpec(memory_space=pltpu.VMEM),) * 4,
        scratch_shapes=scratch,
        compiler_params=pltpu.CompilerParams(
            collective_id=0, has_side_effects=True, vmem_limit_bytes=40 * 1024 * 1024
        ),
    )(*operands)
    results = tuple(pltpu.with_memory_space_constraint(x, pltpu.VMEM) for x in results)
    return pl.pallas_call(
        write_kernel,
        out_shape=(
            jax.ShapeDtypeStruct((4 * rows, 4 * GRID_W, feat), jnp.bfloat16),
            jax.ShapeDtypeStruct((2 * rows, 2 * GRID_W, c_two), jnp.bfloat16),
            jax.ShapeDtypeStruct((rows, GRID_W, c_same), jnp.bfloat16),
        ),
        in_specs=[pl.BlockSpec(memory_space=pltpu.VMEM)] * 4,
        out_specs=(pl.BlockSpec(memory_space=pl.ANY),) * 3,
        scratch_shapes=[
            pltpu.VMEM((rows, GRID_W, c_same), jnp.bfloat16),
            pltpu.SemaphoreType.DMA,
        ],
        compiler_params=pltpu.CompilerParams(vmem_limit_bytes=8 * 1024 * 1024),
    )(*results)


def solution(mesh):
    rows = P(("img", "rows"), None, None)
    return jax.shard_map(
        body,
        mesh=mesh,
        in_specs=(P(None, ("img", "rows"), None),) + (P(),) * 12,
        out_specs=(rows, rows, rows),
        check_vma=False,
    )
```

```python
import functools

import jax
import jax.numpy as jnp
from jax import lax
from jax.experimental import pallas as pl
from jax.experimental.pallas import tpu as pltpu
from jax.sharding import PartitionSpec as P

GRID_W = 64
MESH = pl.DeviceIdType.MESH


def partner(me, step):
    other = me
    bit = 1
    while bit <= step:
        if step & bit:
            other = other + bit * (1 - 2 * lax.rem(lax.div(me, bit), 2))
        bit *= 2
    return other


def dot(left, right):
    return jnp.dot(left, right, preferred_element_type=jnp.float32)


def kernel(
    shards,
    hid_hbm,
    table_hbm,
    w_four_hbm,
    b_four_hbm,
    w_two_hbm,
    b_two_hbm,
    w_same_hbm,
    b_same_hbm,
    up4_hbm,
    up4_b_hbm,
    up2_hbm,
    up2_b_hbm,
    join_hbm,
    joined_ref,
    two_ref,
    same_rows_ref,
    place_ref,
    hid,
    table,
    w_four,
    b_four,
    w_two,
    b_two,
    w_same,
    b_same,
    up4,
    up4_b,
    up2,
    up2_b,
    join,
    stage,
    send_four,
    send_two,
    send_same,
    recv_four,
    recv_two,
    recv_spare,
    edge_out,
    edge_in,
    planes,
    edge_sum,
    joined_f32,
    two_f32,
    load_sem,
    send_sem,
    recv_sem,
    halo_recv_sem,
    relay_sem,
):
    me = lax.axis_index("rows")
    img = lax.axis_index("img")
    tok = hid.shape[1]
    per = tok // shards
    rows = tok // GRID_W
    block = send_four.shape[1]
    split = block // per
    direct = block == 16
    recv_same = same_rows_ref if direct else recv_spare
    group = shards // 4
    plane = lax.div(me, group)
    lower = plane < 2
    last = plane == 3
    beside = plane + 1 - 2 * lax.rem(plane, 2)

    names = (
        (table_hbm, table),
        (hid_hbm.at[0], hid.at[0]),
        (w_four_hbm, w_four),
        (b_four_hbm, b_four),
        (hid_hbm.at[1], hid.at[1]),
        (w_two_hbm, w_two),
        (b_two_hbm, b_two),
        (hid_hbm.at[2], hid.at[2]),
        (w_same_hbm, w_same),
        (b_same_hbm, b_same),
        (up4_hbm, up4),
        (up4_b_hbm, up4_b),
        (join_hbm, join),
        (up2_hbm, up2),
        (up2_b_hbm, up2_b),
    )
    stages = (0, 1, 1, 1, 2, 2, 2, 3, 3, 3, 0, 0, 0, 0, 0)
    loads = [pltpu.make_async_copy(src, dst, load_sem.at[stage_of]) for (src, dst), stage_of in zip(names, stages)]

    for load in loads[:4]:
        load.start()

    def row_in(other_plane, i):
        return partner(me, i) + (other_plane - plane) * group

    barrier = pltpu.get_barrier_semaphore()

    def greet(other_plane, some):
        for i in some:
            pl.semaphore_signal(barrier, inc=1, device_id=(img, row_in(other_plane, i)), device_id_type=MESH)

    @pl.when(~last)
    def _():
        greet(jnp.where(lower, 2, 0), range(group))
        greet(jnp.where(lower, 3, 1), range(group))
        greet(beside, range(group))

    greet(plane, range(1, group))

    for load in loads[4:10]:
        load.start()

    loads[0].wait()
    mine = jnp.broadcast_to(table[pl.ds(me, 1), :].astype(jnp.float32), (tok, tok))
    smaller = (mine.T < mine).astype(jnp.float32)
    slot_row = jnp.sum(smaller, axis=0, keepdims=True)
    down = lax.broadcasted_iota(jnp.int32, (tok, tok), 0)
    across = lax.broadcasted_iota(jnp.int32, (tok, tok), 1)
    shard_row = lax.div(table[pl.ds(me, 1), :], tok).astype(jnp.float32)
    packed_row = slot_row + shard_row * (block - per)
    packed_row = jnp.concatenate([packed_row + part * per for part in range(split)], axis=1)
    packed = lax.broadcasted_iota(jnp.int32, (shards * block, split * tok), 0).astype(jnp.float32)
    scatter = (packed == packed_row).astype(jnp.float32).astype(jnp.bfloat16)

    def project(hook, first, weight, bias, send):
        channels = weight.shape[1]
        for load in loads[first : first + 3]:
            load.wait()
        projected = (dot(hid[hook], weight[...]) + bias[...]).astype(jnp.bfloat16)
        width = channels // split
        stacked = [projected[:, part * width : (part + 1) * width] for part in range(split)]
        ordered = dot(scatter, jnp.concatenate(stacked, axis=0))
        if first == 1:
            for load in loads[10:]:
                load.start()
        if direct:
            send[...] = ordered.astype(jnp.bfloat16).reshape(send.shape)
        else:
            stage[:, :channels] = ordered
            for shard in range(shards):
                send[shard] = stage[shard * per : (shard + 1) * per, :channels].astype(jnp.bfloat16)

    def push(index, send, recv, other):
        pltpu.make_async_remote_copy(
            src_ref=send.at[other],
            dst_ref=recv.at[me],
            send_sem=send_sem,
            recv_sem=recv_sem.at[jnp.where(lower, 0, 1) if index == 0 else index + 1],
            device_id=(img, other),
            device_id_type=MESH,
        ).start()

    def exchange(index, send, recv, other_plane, some):
        for i in reversed(some):
            push(index, send, recv, row_in(other_plane, i))

    def exchange_early(index, send, recv):
        exchange(index, send, recv, jnp.where(lower, 2, 0), range(group))

        @pl.when(~lower)
        def _():
            exchange(index, send, recv, 1, range(group))

        @pl.when(plane != 2)
        def _():
            exchange(index, send, recv, beside, range(group))

        exchange(index, send, recv, plane, range(1, group))
        recv[me] = send[me]

    def bulk_wait(buffer, count, sem):
        part = buffer.at[pl.ds(0, count)]
        pltpu.make_async_copy(part, part, sem).wait()

    def arrive(recv, planes_in, own, sem):
        for mine in (0, 1):

            @pl.when(own == (mine == 1))
            def _():
                bulk_wait(recv, planes_in * group - mine, recv_sem.at[sem])

    def collect(recv):
        width = recv.shape[2]
        if direct:
            return recv[...].reshape(shards * block, width)
        for shard in range(shards):
            stage[shard * per : (shard + 1) * per, :width] = recv[shard].astype(jnp.float32)
        return stage[:, :width].astype(jnp.bfloat16)

    def in_cells(recv):
        tile = dot(place, collect(recv)).astype(jnp.bfloat16)
        return jnp.concatenate([tile[part * tok : (part + 1) * tok] for part in range(split)], axis=1)

    project(0, 1, w_four, b_four, send_four)

    @pl.when(plane >= 2)
    def _():
        pl.semaphore_wait(barrier, jnp.where(last, shards - 1, shards - 1 - group))

        @pl.when(last)
        def _():
            for other_plane in (0, 1, 2):
                to = row_in(other_plane, 0)
                pl.semaphore_signal(relay_sem, inc=1, device_id=(img, to), device_id_type=MESH)

        exchange_early(0, send_four, recv_four)

    project(1, 4, w_two, b_two, send_two)

    @pl.when(plane == 1)
    def _():
        pl.semaphore_wait(barrier, shards - 1 - group)
        exchange_early(0, send_four, recv_four)

    @pl.when(plane > 0)
    def _():
        exchange_early(1, send_two, recv_two)

    project(2, 7, w_same, b_same, send_same)

    @pl.when(plane == 0)
    def _():
        pl.semaphore_wait(barrier, shards - 1 - group)
        exchange_early(0, send_four, recv_four)
        exchange_early(1, send_two, recv_two)

    other_rows = range(group // 2)
    first_rows = range(group // 2, group)

    @pl.when(plane == 1)
    def _():
        exchange(2, send_same, recv_same, 2, first_rows)

    @pl.when(~last)
    def _():
        pl.semaphore_wait(relay_sem, 1)
        exchange(0, send_four, recv_four, 3, range(group))
        exchange(1, send_two, recv_two, 3, range(group))

    spot = lax.rem(me, group)
    faces_beside = jnp.where(lax.rem(plane, 2) == 0, spot == group - 1, spot == 0)

    inner = (plane == 1) | (plane == 2)
    outer = ~inner
    faces_across = ((plane == 1) & (spot == group - 1)) | ((plane == 2) & (spot == 0))

    def same_far(some, rows_to=range(group)):
        @pl.when(some)
        def _():
            exchange(2, send_same, recv_same, jnp.where(lower, 3, 0), rows_to)

    def same_beside(some):
        @pl.when(some)
        def _():
            exchange(2, send_same, recv_same, beside, range(group))

    def same_across(some):
        @pl.when(some & (plane != 1))
        def _():
            exchange(2, send_same, recv_same, jnp.where(lower, 2, 1), first_rows)

        @pl.when(some)
        def _():
            exchange(2, send_same, recv_same, jnp.where(lower, 2, 1), other_rows)

    same_far(inner)
    same_beside(inner)
    same_across(inner & ~faces_across)
    exchange(2, send_same, recv_same, plane, range(1, group))
    recv_same[me] = send_same[me]

    wanted = down + me * tok
    source = jnp.zeros((tok, tok), jnp.float32)
    for shard in range(1, shards):
        source = source + jnp.where(table[shard : shard + 1, :] == wanted, float(shard), 0.0)
    source = jnp.broadcast_to(jnp.sum(source, axis=1, keepdims=True), (tok, tok))
    earlier = jnp.where((source == source.T) & (across < down), 1.0, 0.0)
    slot_col = source[:, :1] * block + jnp.sum(earlier, axis=1, keepdims=True)
    slot_col = jnp.concatenate([slot_col + part * per for part in range(split)], axis=0)
    packed = lax.broadcasted_iota(jnp.int32, (split * tok, shards * block), 1).astype(jnp.float32)
    place = (packed == slot_col).astype(jnp.float32).astype(jnp.bfloat16)
    place_ref[...] = place

    arrive(recv_four, 2, ~lower, 1)
    same_far(last)
    same_beside(last)
    same_across(last)
    arrive(recv_four, 2, lower, 0)
    free = (plane == 0) & ~faces_beside
    same_far(free)
    same_beside(free)
    same_across(free)
    tile_four = in_cells(recv_four)
    edge_out[0] = tile_four[:GRID_W]
    edge_out[1] = tile_four[tok - GRID_W :]

    def halo(side):
        return pltpu.make_async_remote_copy(
            src_ref=edge_out.at[1 - side],
            dst_ref=edge_in.at[side],
            send_sem=send_sem,
            recv_sem=halo_recv_sem.at[side],
            device_id=(img, me + 1 if side == 0 else me - 1),
            device_id_type=MESH,
        )

    has_below = me < shards - 1
    has_above = me > 0

    @pl.when(has_below)
    def _():
        halo(0).start()

    @pl.when(has_above)
    def _():
        halo(1).start()

    facing = (plane == 0) & faces_beside
    same_far(facing)
    same_beside((plane == 0) & faces_beside)
    same_across(faces_across | facing)

    column = lax.broadcasted_iota(jnp.int32, (GRID_W, 1), 0)
    c_up = join.shape[0] // 9

    def put_row(row, phase, values):
        where = pl.ds((row + 1) * GRID_W, GRID_W)
        planes[phase + 1, where, :] = values.astype(jnp.bfloat16)
        if phase == 3:
            moved = jnp.where(column == 0, 0.0, pltpu.roll(values, 1, axis=0))
            planes[0, where, :] = moved.astype(jnp.bfloat16)
        if phase == 0:
            moved = jnp.where(column == GRID_W - 1, 0.0, pltpu.roll(values, GRID_W - 1, axis=0))
            planes[5, where, :] = moved.astype(jnp.bfloat16)

    for load in loads[10:]:
        load.wait()
    for a in range(4):
        for b in range(4):
            tap = a * 4 + b
            value = dot(tile_four, up4[:, tap * c_up : (tap + 1) * c_up]) + up4_b[...]
            for i in range(rows):
                put_row(4 * i + a, b, value[i * GRID_W : (i + 1) * GRID_W])

    half = joined_ref.shape[2] // 2

    def join_rows(jobs, count):
        windows = [
            jnp.concatenate(
                [
                    planes[phase + col, pl.ds((first + row) * GRID_W, count * GRID_W), :]
                    for row in range(3)
                    for col in range(3)
                ],
                axis=1,
            )
            for phase, first in jobs
        ]
        total = dot(jnp.concatenate(windows, axis=0), join[...])
        for job, (phase, first) in enumerate(jobs):
            for r in range(count):
                at = (job * count + r) * GRID_W
                for h in range(2):
                    joined_f32[first + r, h, pl.ds(phase, GRID_W, stride=4), :] = total[
                        at : at + GRID_W, h * half : (h + 1) * half
                    ]

    def finish_rows(first, count):
        for r in range(first, first + count):
            for h in range(2):
                joined_ref[r, :, h * half : (h + 1) * half] = joined_f32[r, h].astype(jnp.bfloat16)

    out_rows = 4 * rows
    for phase in range(4):
        join_rows([(phase, 1)], out_rows - 2)
    finish_rows(1, out_rows - 2)

    bulk_wait(recv_two, shards - 1, recv_sem.at[2])
    tile_two = in_cells(recv_two)
    c_two = two_ref.shape[2]
    for a in range(2):
        for b in range(2):
            tap = a * 2 + b
            value = dot(tile_two, up2[:, tap * c_two : (tap + 1) * c_two]) + up2_b[...]
            for i in range(rows):
                for h in range(c_two // 128):
                    two_f32[2 * i + a, h, pl.ds(b, GRID_W, stride=2), :] = value[
                        i * GRID_W : (i + 1) * GRID_W, h * 128 : (h + 1) * 128
                    ]
    for r in range(2 * rows):
        for h in range(c_two // 128):
            two_ref[r, :, h * 128 : (h + 1) * 128] = two_f32[r, h].astype(jnp.bfloat16)

    def edge_product(first, tap_rows):
        windows = [
            jnp.concatenate(
                [
                    planes[phase + col, pl.ds((first + row) * GRID_W, GRID_W), :]
                    for row in tap_rows
                    for col in range(3)
                ],
                axis=1,
            )
            for phase in range(4)
        ]
        weights = join[tap_rows[0] * 3 * c_up : (tap_rows[-1] + 1) * 3 * c_up, :]
        return dot(jnp.concatenate(windows, axis=0), weights)

    borders = ((0, (1, 2), (0,)), (out_rows - 1, (0, 1), (2,)))
    for side, (first, inside, beyond) in enumerate(borders):
        edge_sum[side] = edge_product(first, inside)

    @pl.when(has_below)
    def _():
        halo(1).wait_recv()

    @pl.when(has_above)
    def _():
        halo(0).wait_recv()

    for side, present, a, row in ((0, has_above, 3, -1), (1, has_below, 0, out_rows)):
        for b in range(4):
            tap = a * 4 + b
            value = dot(edge_in[side], up4[:, tap * c_up : (tap + 1) * c_up]) + up4_b[...]
            put_row(row, b, jnp.where(present, value, 0.0))
    for side, (first, inside, beyond) in enumerate(borders):
        total = edge_sum[side] + edge_product(first, beyond)
        for phase in range(4):
            for h in range(2):
                joined_f32[first, h, pl.ds(phase, GRID_W, stride=4), :] = total[
                    phase * GRID_W : (phase + 1) * GRID_W, h * half : (h + 1) * half
                ]
    finish_rows(0, 1)
    finish_rows(out_rows - 1, 1)

    bulk_wait(recv_same, shards - 1, recv_sem.at[3])
    if not direct:
        same_rows_ref[...] = collect(recv_same)

    for send in (send_four, send_two, send_same):
        bulk_wait(send, shards - 1, send_sem)

    @pl.when(has_below)
    def _():
        halo(0).wait_send()

    @pl.when(has_above)
    def _():
        halo(1).wait_send()


def write_kernel(joined_ref, two_ref, same_rows_ref, place_ref, joined_out, two_out, same_out, same, sem):
    copies = [
        pltpu.make_async_copy(src.at[pl.ds(i, 1)], dst.at[pl.ds(i, 1)], sem)
        for src, dst in ((joined_ref, joined_out), (two_ref, two_out))
        for i in range(src.shape[0])
    ]
    for copy in copies:
        copy.start()
    arrived = same_rows_ref[...]
    width = arrived.shape[-1]
    tile = dot(place_ref[...], arrived.reshape(-1, width)).astype(jnp.bfloat16)
    tok = same.shape[0] * GRID_W
    for part in range(same.shape[2] // width):
        for i in range(same.shape[0]):
            at = part * tok + i * GRID_W
            same[i, :, part * width : (part + 1) * width] = tile[at : at + GRID_W]
    copies.append(pltpu.make_async_copy(same, same_out, sem))
    copies[-1].start()
    for copy in copies:
        copy.wait()


def body(
    hidden_states,
    cell_of,
    proj_four_weight,
    proj_four_bias,
    proj_two_weight,
    proj_two_bias,
    proj_same_weight,
    proj_same_bias,
    up4_weight,
    up4_bias,
    up2_weight,
    up2_bias,
    join_weight,
):
    tok = hidden_states.shape[1]
    shards = lax.axis_size("rows")
    per = tok // shards
    rows = tok // GRID_W
    operands = (
        hidden_states,
        cell_of.reshape(shards, tok),
        proj_four_weight,
        proj_four_bias[None, :],
        proj_two_weight,
        proj_two_bias[None, :],
        proj_same_weight,
        proj_same_bias[None, :],
        up4_weight,
        up4_bias[None, :],
        up2_weight,
        up2_bias[None, :],
        join_weight.reshape(-1, join_weight.shape[3]),
    )
    c_four = proj_four_weight.shape[1]
    c_two = proj_two_weight.shape[1]
    c_same = proj_same_weight.shape[1]
    feat = join_weight.shape[3]
    widths = (c_four, c_two, c_same)
    direct = 16 % per == 0 and all(c * per % (16 * 128) == 0 for c in widths)
    block = 16 if direct else per
    split = block // per
    wire = [pltpu.VMEM((shards, block, c // split), jnp.bfloat16) for c in widths]
    spare = pltpu.VMEM((8, 128), jnp.bfloat16) if direct else wire[2]
    arrived = wire[2].shape if direct else (tok, c_same)
    scratch = [pltpu.VMEM(x.shape, x.dtype) for x in operands]
    scratch += [pltpu.VMEM((tok, max(widths)), jnp.float32)]
    scratch += wire + wire[:2] + [spare]
    scratch += [
        pltpu.VMEM((2, GRID_W, c_four), jnp.bfloat16),
        pltpu.VMEM((2, GRID_W, c_four), jnp.bfloat16),
        pltpu.VMEM((6, (4 * rows + 2) * GRID_W, c_four), jnp.bfloat16),
        pltpu.VMEM((2, 4 * GRID_W, feat), jnp.float32),
        pltpu.VMEM((4 * rows, 2, 4 * GRID_W, feat // 2), jnp.float32),
        pltpu.VMEM((2 * rows, c_two // 128, 2 * GRID_W, 128), jnp.float32),
        pltpu.SemaphoreType.DMA((4,)),
        pltpu.SemaphoreType.DMA,
        pltpu.SemaphoreType.DMA((4,)),
        pltpu.SemaphoreType.DMA((2,)),
        pltpu.SemaphoreType.REGULAR,
    ]
    operands = tuple(pltpu.with_memory_space_constraint(x, pltpu.HBM) for x in operands)
    results = pl.pallas_call(
        functools.partial(kernel, shards),
        out_shape=(
            pltpu.VMEM((4 * rows, 4 * GRID_W, feat), jnp.bfloat16),
            pltpu.VMEM((2 * rows, 2 * GRID_W, c_two), jnp.bfloat16),
            pltpu.VMEM(arrived, jnp.bfloat16),
            pltpu.VMEM((split * tok, shards * block), jnp.bfloat16),
        ),
        in_specs=[pl.BlockSpec(memory_space=pl.ANY)] * len(operands),
        out_specs=(pl.BlockSpec(memory_space=pltpu.VMEM),) * 4,
        scratch_shapes=scratch,
        compiler_params=pltpu.CompilerParams(
            collective_id=0, has_side_effects=True, vmem_limit_bytes=40 * 1024 * 1024
        ),
    )(*operands)
    results = tuple(pltpu.with_memory_space_constraint(x, pltpu.VMEM) for x in results)
    return pl.pallas_call(
        write_kernel,
        out_shape=(
            jax.ShapeDtypeStruct((4 * rows, 4 * GRID_W, feat), jnp.bfloat16),
            jax.ShapeDtypeStruct((2 * rows, 2 * GRID_W, c_two), jnp.bfloat16),
            jax.ShapeDtypeStruct((rows, GRID_W, c_same), jnp.bfloat16),
        ),
        in_specs=[pl.BlockSpec(memory_space=pltpu.VMEM)] * 4,
        out_specs=(pl.BlockSpec(memory_space=pl.ANY),) * 3,
        scratch_shapes=[
            pltpu.VMEM((rows, GRID_W, c_same), jnp.bfloat16),
            pltpu.SemaphoreType.DMA,
        ],
        compiler_params=pltpu.CompilerParams(vmem_limit_bytes=8 * 1024 * 1024),
    )(*results)


def solution(mesh):
    rows = P(("img", "rows"), None, None)
    return jax.shard_map(
        body,
        mesh=mesh,
        in_specs=(P(None, ("img", "rows"), None),) + (P(),) * 12,
        out_specs=(rows, rows, rows),
        check_vma=False,
    )
```
